8 devices in a mesh: dp: 1 (over z), tp: 2 (over y), ep: 4 (over x, core).
Axes of the slice: x: 2, y: 2, z: 1, core: 2. Of those that a mesh axis runs over, the one named last changes fastest.
Arguments:
- x: bfloat16 [256, 2048], P(('dp', 'tp', 'ep'))
- route_idx: int32 [256, 8], P(('dp', 'tp', 'ep'))
- gates: float32 [256, 8], P(('dp', 'tp', 'ep'))
- w1: bfloat16 [128, 2048, 768], P('ep', None, 'tp')
- w3: bfloat16 [128, 2048, 768], P('ep', None, 'tp')
- w2: bfloat16 [128, 768, 2048], P('ep', 'tp')
Outputs:
- output: bfloat16 [256, 2048], P(('dp', 'tp', 'ep'))
All inputs are finite; a program needn't handle non-finite values.
Results may differ from the reference program's by a relative error of at most 0.00783045.
Values are sent between devices in bfloat16 or wider.
A program may use at most 1 GiB of HBM per device.

```python
import jax
import jax.numpy as jnp
from jax import lax

D = 2048
E = 128
F = 768
TOP = 8
T_LOC = 32
GROUP = 8
N_TOK = GROUP * T_LOC
CAP = T_LOC // 2


def device_routes(key, z):
    kn, kp, ks = jax.random.split(key, 3)
    q = jax.nn.softmax(z + 0.5 * jax.random.normal(kn, (E,), jnp.float32))
    lim = (CAP - 2) / (TOP * T_LOC)
    p1 = jnp.minimum(q, lim)
    room = lim - p1
    p = p1 + (1.0 - jnp.sum(p1)) * room / jnp.maximum(jnp.sum(room), 1e-9)
    total = TOP * T_LOC
    bounds = jnp.floor(total * jnp.cumsum(p)[:-1]).astype(jnp.int32)
    ids = jnp.sum((jnp.arange(total)[:, None] >= bounds[None, :]).astype(jnp.int32), axis=1)
    route = ids.reshape(TOP, T_LOC).T
    route = route[jax.random.permutation(kp, T_LOC)]
    order = jnp.argsort(jax.random.uniform(ks, (T_LOC, TOP), jnp.float32), axis=1)
    return jnp.take_along_axis(route, order, axis=1).astype(jnp.int32)


def setup_inputs(seed: int = 0, part: int = 0) -> dict:
    kpart = jax.random.fold_in(jax.random.key(seed), part)
    kx, kr, kg, kh = jax.random.split(kpart, 4)
    k1, k3, k2 = jax.random.split(jax.random.key(seed + 1), 3)
    x = jax.random.normal(kx, (N_TOK, D), jnp.float32).astype(jnp.bfloat16)
    hot = 1.5 * jax.random.normal(kh, (E,), jnp.float32)
    route_idx = jax.vmap(lambda k: device_routes(k, hot))(jax.random.split(kr, GROUP)).reshape(N_TOK, TOP)
    gates = jax.random.uniform(kg, (N_TOK, TOP), jnp.float32, 0.5, 1.5) * TOP ** -0.5
    w1 = (jax.random.normal(k1, (E, D, F), jnp.float32) * D ** -0.5).astype(jnp.bfloat16)
    w3 = (jax.random.normal(k3, (E, D, F), jnp.float32) * D ** -0.5).astype(jnp.bfloat16)
    w2 = (jax.random.normal(k2, (E, F, D), jnp.float32) * F ** -0.5).astype(jnp.bfloat16)
    return {'x': x, 'route_idx': route_idx, 'gates': gates, 'w1': w1, 'w3': w3, 'w2': w2}


def reference(x, route_idx, gates, w1, w3, w2):
    n_tok = x.shape[0]
    cap_e = n_tok // 2
    xp = jnp.concatenate([x, jnp.zeros((1, D), x.dtype)], axis=0)
    tok = jnp.arange(n_tok, dtype=jnp.int32)

    def body(acc, inp):
        e, a1, a3, a2 = inp
        sel = route_idx == e
        wt = jnp.sum(jnp.where(sel, gates, 0.0), axis=1)
        m = jnp.any(sel, axis=1)
        pos = jnp.where(m, jnp.cumsum(m.astype(jnp.int32)) - 1, cap_e)
        idx = jnp.full((cap_e,), n_tok, jnp.int32).at[pos].set(tok, mode='drop')
        xs = xp[idx]
        a = jnp.dot(xs, a1, preferred_element_type=jnp.float32)
        b = jnp.dot(xs, a3, preferred_element_type=jnp.float32)
        h = (jax.nn.silu(a) * b).astype(jnp.bfloat16)
        o = jnp.dot(h, a2, preferred_element_type=jnp.float32).astype(jnp.bfloat16)
        op = jnp.concatenate([o, jnp.zeros((1, D), o.dtype)], axis=0)
        return acc + op[pos].astype(jnp.float32) * wt[:, None], None

    acc, _ = lax.scan(body, jnp.zeros((n_tok, D), jnp.float32), (jnp.arange(E, dtype=jnp.int32), w1, w3, w2))
    return acc.astype(jnp.bfloat16)
```

```python
import functools

import jax
import jax.numpy as jnp
from jax import lax
from jax.experimental import pallas as pl
from jax.experimental.pallas import tpu as pltpu
from jax.sharding import PartitionSpec as P

MESH = pl.DeviceIdType.MESH
F32 = jnp.float32
BF16 = jnp.bfloat16
BIG = 1e9


def dot(a, b):
    return jnp.dot(a, b, preferred_element_type=F32)


def iota(shape, dim):
    return lax.broadcasted_iota(jnp.int32, shape, dim)


def split3(g):
    g1 = g.astype(BF16)
    r = g - g1.astype(F32)
    g2 = r.astype(BF16)
    g3 = (r - g2.astype(F32)).astype(BF16)
    return g1, g2, g3


def moe_kernel(b, flush, fb, depth, ring, *refs):
    (base_ref, x_ref, route_ref, gates_ref, w1_ref, w3_ref, w2_ref, y_ref, need_ref,
     x_all, r_all, g_all, code, gm, tab_v, tab_s, w1b, w3b, w2b, o_buf, send, recv, y_acc, y_recv,
     gs_sem, gr_sem, tab_sem, w_sem, s_sem, r_sem, fs_sem, fr_sem, ys_sem, yr_sem, fsend) = refs
    tp = lax.axis_index("tp")
    ep = lax.axis_index("ep")
    t_loc, d = x_ref.shape
    n_e = w1_ref.shape[0]
    half = 4 * t_loc
    n_main = n_e * b
    n_rows = n_main + flush
    lag = 4
    peer = {"tp": lax.rem(tp + 1, 2), "ep": ep}

    def weights(e, slot):
        return [pltpu.make_async_copy(w1_ref.at[e], w1b.at[slot], w_sem.at[0, slot]),
                pltpu.make_async_copy(w3_ref.at[e], w3b.at[slot], w_sem.at[1, slot]),
                pltpu.make_async_copy(w2_ref.at[e], w2b.at[slot], w_sem.at[2, slot])]

    for e in range(depth):
        for c in weights(e, e):
            c.start()

    others = [(dt, de) for dt in range(2) for de in range(4) if (dt, de) != (0, 0)]

    def device(dt, de):
        return {"tp": lax.rem(tp + dt, 2), "ep": lax.rem(ep + de, 4)}

    barrier = pltpu.get_barrier_semaphore()
    for dt, de in others:
        pl.semaphore_signal(barrier, inc=1, device_id=device(dt, de), device_id_type=MESH)
    pl.semaphore_wait(barrier, len(others))

    def gather(kind, dt, de):
        src, dst = ((route_ref, r_all), (gates_ref, g_all), (x_ref, x_all))[kind]
        row = pl.multiple_of(dt * half + ep * t_loc, t_loc)
        return pltpu.make_async_remote_copy(
            src_ref=src, dst_ref=dst.at[pl.ds(row, t_loc)], send_sem=gs_sem.at[kind, dt * 4 + de],
            recv_sem=gr_sem.at[kind, dt * 4 + de], device_id=device(dt, de), device_id_type=MESH)

    for kind in range(3):
        for dt, de in others:
            gather(kind, dt, de).start()
    mine = pl.ds(pl.multiple_of(ep * t_loc, t_loc), t_loc)
    r_all[mine, :] = route_ref[...]
    g_all[mine, :] = gates_ref[...]
    x_all[mine, :] = x_ref[...]
    for kind in range(2):
        for dt, de in others:
            gather(kind, dt, de).wait()

    n_tok = 2 * half
    lane = iota((n_tok, 128), 1)
    route = r_all[...]
    gates = g_all[...]
    hit_all = jnp.zeros((n_tok, 128), F32)
    hit = jnp.zeros((n_tok, 128), F32)
    gate = jnp.zeros((half, 128), F32)
    for k in range(route.shape[1]):
        col = route[:, k:k + 1]
        hit_all = jnp.where(col == lane, 1.0, hit_all)
        rel = (col - ep * n_e == lane) & (lane < n_e)
        hit = jnp.where(rel, 1.0, hit)
        gate = jnp.where(rel[:half], gates[:half, k:k + 1], gate)
    cnt_a = jnp.sum(hit_all[:half], axis=0, keepdims=True) - b
    cnt_b = jnp.sum(hit_all[half:], axis=0, keepdims=True) - b
    row16 = iota((16, 128), 0)
    cnt = jnp.where(row16 == 0, cnt_a, jnp.where(row16 == 1, cnt_b, -float(b)))
    k_i, s_i = iota((128, 128), 0), iota((128, 128), 1)
    suffix = ((k_i >= s_i) & (k_i // n_e == s_i // n_e)).astype(BF16)
    need_ref[...] = jnp.max(jnp.max(dot(cnt.astype(BF16), suffix), axis=1, keepdims=True), axis=0, keepdims=True) + jnp.zeros((8, 128), F32)

    t_i, u_i = iota((n_tok, n_tok), 0), iota((n_tok, n_tok), 1)
    before = ((t_i < u_i) & (t_i // half == u_i // half)).astype(BF16)
    hit_t = jnp.transpose(hit)[:n_e, :]
    pos_t = dot(hit_t.astype(BF16), before)
    code[...] = jnp.where(hit_t > 0, pos_t + jnp.where(iota((n_e, n_tok), 1) >= half, float(half // 2), 0.0), -1.0)
    h_i, v_i = iota((half, half), 0), iota((half, half), 1)
    pos = dot((v_i < h_i).astype(BF16), hit[:half].astype(BF16))
    upto = (iota((n_e, n_e), 1) <= iota((n_e, n_e), 0)).astype(BF16)

    k_f = iota((n_e, n_rows), 0).astype(F32)
    i_row = iota((1, n_rows), 1)
    if b:
        step = jnp.where(i_row < n_main, i_row // b, n_e).astype(F32)
        off = jnp.where(i_row < n_main, lax.rem(i_row, b), i_row - n_main).astype(F32)
    else:
        step = jnp.full((1, n_rows), float(n_e), F32)
        off = i_row.astype(F32)

    def table(count, shift):
        c = dot(upto, (count + jnp.zeros((n_e, 128), F32)).astype(BF16))[:, :1]
        total = jnp.max(c, axis=0, keepdims=True)

        def served(m):
            inner = jnp.min(jnp.where(k_f <= m, c + b * (m - k_f), BIG), axis=0, keepdims=True)
            return jnp.minimum(inner, b * (m + 1.0))

        q = served(step - 1.0) + off + base_ref[0].astype(F32)
        end = jnp.where(i_row < n_main, served(step), total)
        valid = q < end
        past = c <= q
        expert = jnp.sum(jnp.where(past, 1.0, 0.0), axis=0, keepdims=True)
        rank = q - jnp.max(jnp.where(past, c, 0.0), axis=0, keepdims=True)
        idx = jnp.where(valid, expert * half + rank + shift, 0.0)
        return idx.astype(jnp.int32), expert, rank, valid

    cnt_a = jnp.sum(hit_t[:, :half], axis=1, keepdims=True)
    cnt_b = jnp.sum(hit_t[:, half:], axis=1, keepdims=True)
    idx_b, _, _, _ = table(cnt_b, float(half // 2))
    idx_a, expert, rank, valid = table(cnt_a, 0.0)
    r8 = iota((8, n_rows), 0)
    tab_v[...] = jnp.where(r8 == 0, idx_b, idx_a)
    to_smem = pltpu.make_async_copy(tab_v, tab_s, tab_sem)
    to_smem.start()
    one = jnp.where((iota((128, n_rows), 0).astype(F32) == expert) & valid, 1.0, 0.0).astype(BF16)
    same = dot(pos.astype(BF16), one) == rank
    for j, g in enumerate(split3(gate)):
        full = jnp.where(same, dot(g, one), 0.0).astype(BF16)
        for m in range(n_rows // 128):
            gm[m, j] = full[:, m * 128:(m + 1) * 128]
    y_acc[...] = jnp.zeros_like(y_acc)
    to_smem.wait()
    for dt, de in others:
        gather(2, dt, de).wait()

    def chunk(e):
        slot = lax.rem(e, ring)
        return pltpu.make_async_remote_copy(
            src_ref=send.at[slot], dst_ref=recv.at[pl.ds(pl.multiple_of(e * b, b), b)], send_sem=s_sem.at[slot],
            recv_sem=r_sem.at[e], device_id=peer, device_id_type=MESH)

    def piece(f):
        return pltpu.make_async_remote_copy(
            src_ref=fsend.at[pl.ds(pl.multiple_of(f * fb, fb), fb)],
            dst_ref=recv.at[pl.ds(pl.multiple_of(n_main + f * fb, fb), fb)], send_sem=fs_sem.at[f],
            recv_sem=fr_sem.at[f], device_id=peer, device_id_type=MESH)


    def partial(way, i):
        return o_buf[pl.ds(jnp.clip(tab_s[way, i], 0, n_e * half - 1), 1), :]

    def add_own(first, rows):
        for r in range(rows):
            i = first + r
            recv[pl.ds(i, 1), :] = recv[pl.ds(i, 1), :] + partial(1, i)

    def combine(m):
        o = recv[pl.ds(pl.multiple_of(m * 128, 128), 128), :].astype(BF16)
        y_acc[...] += dot(gm[m, 0], o) + dot(gm[m, 1], o) + dot(gm[m, 2], o)

    slot_i = iota((half, n_tok), 0).astype(F32)

    @pl.loop(0, n_e)
    def _(e):
        slot = lax.rem(e, depth)
        pick = jnp.where(code[pl.ds(e, 1), :] == slot_i, 1.0, 0.0).astype(BF16)
        xs = dot(pick, x_all[...]).astype(BF16)
        c1, c3, c2 = weights(e, slot)
        c1.wait()
        u = dot(xs, w1b[slot])
        c3.wait()
        v = dot(xs, w3b[slot])
        h = (u * jax.nn.sigmoid(u) * v).astype(BF16)
        c2.wait()
        o_buf[pl.ds(pl.multiple_of(e * half, half), half), :] = dot(h, w2b[slot])

        @pl.when(e + depth < n_e)
        def _():
            for c in weights(e + depth, slot):
                c.start()

        if b:
            @pl.when(e >= ring)
            def _():
                chunk(e - ring).wait_send()

            s = lax.rem(e, ring)
            for r in range(b):
                send[s, r:r + 1, :] = partial(0, e * b + r)
            chunk(e).start()

            @pl.when(e >= lag)
            def _():
                chunk(e - lag).wait_recv()
                add_own((e - lag) * b, b)

            for m in range(n_main // 128 - 1):
                @pl.when(e == (m + 1) * 128 // b - 1 + lag)
                def _():
                    combine(m)

    @pl.loop(0, flush // fb)
    def _(f):
        @pl.loop(0, fb)
        def _(r):
            i = f * fb + r
            fsend[pl.ds(i, 1), :] = partial(0, n_main + i)
        piece(f).start()

    if b:
        @pl.loop(n_e - lag, n_e)
        def _(e):
            chunk(e).wait_recv()
            add_own(e * b, b)
        combine(n_main // 128 - 1)

        @pl.loop(n_e - ring, n_e)
        def _(e):
            chunk(e).wait_send()

    @pl.loop(0, flush // fb)
    def _(f):
        piece(f).wait_recv()

        @pl.loop(0, fb)
        def _(r):
            i = n_main + f * fb + r
            recv[pl.ds(i, 1), :] = recv[pl.ds(i, 1), :] + partial(1, i)

    for m in range(n_main // 128, n_rows // 128):
        combine(m)

    @pl.loop(0, flush // fb)
    def _(f):
        piece(f).wait_send()

    def give(o):
        to = lax.rem(ep + o, 4)
        return pltpu.make_async_remote_copy(
            src_ref=y_acc.at[pl.ds(pl.multiple_of(to * t_loc, t_loc), t_loc)], dst_ref=y_recv.at[3 - o],
            send_sem=ys_sem.at[o - 1], recv_sem=yr_sem.at[3 - o], device_id={"tp": tp, "ep": to}, device_id_type=MESH)

    for o in (2, 1, 3):
        give(o).start()
    y = y_acc[mine, :]
    for o in (1, 3, 2):
        give(o).wait_recv()
        y = y + y_recv[3 - o]
    y_ref[...] = y.astype(y_ref.dtype)
    for o in (1, 2, 3):
        give(o).wait_send()


def moe_call(b, flush, fb, depth, ring, out_dtype, cid, base, x, route, gates, w1, w3, w2):
    t_loc, d = x.shape
    n_e, _, f = w1.shape
    n_rows = n_e * b + flush
    half = 4 * t_loc
    dma = pltpu.SemaphoreType.DMA
    vm = pl.BlockSpec(memory_space=pltpu.VMEM)
    hbm = pl.BlockSpec(memory_space=pl.ANY)
    return pl.pallas_call(
        functools.partial(moe_kernel, b, flush, fb, depth, ring),
        out_shape=(jax.ShapeDtypeStruct((t_loc, d), out_dtype), jax.ShapeDtypeStruct((8, 128), F32)),
        in_specs=[pl.BlockSpec(memory_space=pltpu.SMEM), vm, vm, vm, hbm, hbm, hbm],
        out_specs=(vm, vm),
        scratch_shapes=[
            pltpu.VMEM((2 * half, d), BF16),
            pltpu.VMEM((2 * half, route.shape[1]), jnp.int32),
            pltpu.VMEM((2 * half, route.shape[1]), F32),
            pltpu.VMEM((n_e, 2 * half), F32),
            pltpu.VMEM((n_rows // 128, 3, half, 128), BF16),
            pltpu.VMEM((8, n_rows), jnp.int32),
            pltpu.SMEM((8, n_rows), jnp.int32),
            pltpu.VMEM((depth, d, f), BF16),
            pltpu.VMEM((depth, d, f), BF16),
            pltpu.VMEM((depth, f, d), BF16),
            pltpu.VMEM((n_e * half, d), F32),
            pltpu.VMEM((ring, max(b, 8), d), F32),
            pltpu.VMEM((n_rows, d), F32),
            pltpu.VMEM((half, d), F32),
            pltpu.VMEM((3, t_loc, d), F32),
            dma((3, 8)), dma((3, 8)), dma, dma((3, depth)), dma((ring,)), dma((n_e,)),
            dma((flush // fb,)), dma((flush // fb,)), dma((3,)), dma((3,)),
            pltpu.VMEM((flush, d), F32),
        ],
        compiler_params=pltpu.CompilerParams(collective_id=cid, has_side_effects=True, vmem_limit_bytes=67043328),
    )(base, x, route, gates, w1, w3, w2)


FLUSH = 128


def solution(mesh):
    tok_spec = P(('dp', 'tp', 'ep'), None)

    def local(x, route_idx, gates, w1, w3, w2):
        zero = jnp.zeros((1,), jnp.int32)
        y, need = moe_call(8, FLUSH, 16, 3, 4, BF16, 1, zero, x, route_idx, gates, w1, w3, w2)

        def slow(_):
            part = 256
            total = jnp.zeros(x.shape, F32)

            def one(p, acc):
                base = jnp.full((1,), p * part, jnp.int32)
                return acc + moe_call(0, part, 16, 3, 4, F32, 2, base, x, route_idx, gates, w1, w3, w2)[0]

            return lax.fori_loop(0, 1024 // part, one, total).astype(BF16)

        return lax.cond(need[0, 0] > FLUSH, slow, lambda y: y, y)

    return jax.shard_map(local, mesh=mesh,
                         in_specs=(tok_spec, tok_spec, tok_spec, P('ep', None, 'tp'), P('ep', None, 'tp'), P('ep', 'tp', None)),
                         out_specs=tok_spec, check_vma=False)
```

```python
import functools

import jax
import jax.numpy as jnp
from jax import lax
from jax.experimental import pallas as pl
from jax.experimental.pallas import tpu as pltpu
from jax.sharding import PartitionSpec as P

MESH = pl.DeviceIdType.MESH
F32 = jnp.float32
BF16 = jnp.bfloat16
BIG = 1e9


def dot(a, b):
    return jnp.dot(a, b, preferred_element_type=F32)


def iota(shape, dim):
    return lax.broadcasted_iota(jnp.int32, shape, dim)


def split3(g):
    g1 = g.astype(BF16)
    r = g - g1.astype(F32)
    g2 = r.astype(BF16)
    g3 = (r - g2.astype(F32)).astype(BF16)
    return g1, g2, g3


def moe_kernel(b, rows_part, cols_part, fb, nb, depth, ring, *refs):
    (base_ref, x_ref, route_ref, gates_ref, w1_ref, w3_ref, w2_ref, y_ref, need_ref,
     x_all, r_all, g_all, before, code, gm, tab_v, tab_s, w1b, w3b, w2b, o_buf, send, fsend, recv, own, y_acc, y_recv,
     gs_sem, gr_sem, xs_sem, xr_sem, tab_sem, w_sem, s_sem, r_sem, fs_sem, fr_sem, cs_sem, cr_sem, ys_sem, yr_sem) = refs
    tp = lax.axis_index("tp")
    ep = lax.axis_index("ep")
    t_loc, d = x_ref.shape
    n_e = w1_ref.shape[0]
    half = 4 * t_loc
    n_tok = 2 * half
    flush = rows_part + cols_part
    n_main = n_e * b
    n_rows = n_main + flush
    lag = 4
    wide = d // nb
    tp_peer = lax.rem(tp + 1, 2)
    ep_x = lax.rem(ep + 2, 4)
    ep_c = ep + 1 - 2 * lax.rem(ep, 2)
    ep_d = lax.rem(ep_c + 2, 4)
    peer = {"tp": tp_peer, "ep": ep}
    dev_x = {"tp": tp, "ep": ep_x}
    dev_c = {"tp": tp, "ep": ep_c}

    def weights(e, slot):
        return [pltpu.make_async_copy(w1_ref.at[e], w1b.at[slot], w_sem.at[0, slot]),
                pltpu.make_async_copy(w3_ref.at[e], w3b.at[slot], w_sem.at[1, slot]),
                pltpu.make_async_copy(w2_ref.at[e], w2b.at[slot], w_sem.at[2, slot])]

    for e in range(depth):
        for c in weights(e, e):
            c.start()

    others = [(dt, de) for dt in range(2) for de in range(4) if (dt, de) != (0, 0)]

    def device(dt, de):
        return {"tp": lax.rem(tp + dt, 2), "ep": lax.rem(ep + de, 4)}

    barrier = pltpu.get_barrier_semaphore()
    for dt, de in others:
        pl.semaphore_signal(barrier, inc=1, device_id=device(dt, de), device_id_type=MESH)

    t_i, u_i = iota((n_tok, n_tok), 0), iota((n_tok, n_tok), 1)
    before[...] = jnp.where((t_i < u_i) & ((t_i < half) == (u_i < half)), 1.0, 0.0).astype(BF16)
    y_acc[...] = jnp.zeros_like(y_acc)
    pl.semaphore_wait(barrier, len(others))

    def gather(kind, dt, de):
        src, dst = ((route_ref, r_all), (gates_ref, g_all))[kind]
        return pltpu.make_async_remote_copy(
            src_ref=src, dst_ref=dst.at[dt * 4 + ep], send_sem=gs_sem.at[kind, dt * 4 + de],
            recv_sem=gr_sem.at[kind, dt * 4 + de], device_id=device(dt, de), device_id_type=MESH)

    def rows_of(first, n):
        return x_all.at[pl.ds(pl.multiple_of(first, 16), n)]

    def x_copy(i, src, dst, to):
        return pltpu.make_async_remote_copy(src_ref=src, dst_ref=dst, send_sem=xs_sem.at[i], recv_sem=xr_sem.at[i],
                                            device_id=to, device_id_type=MESH)

    near, far, h_loc = ep * t_loc, half + ep * t_loc, t_loc // 2
    x_own = [x_copy(0, x_ref, rows_of(near, t_loc), dev_c),
             x_copy(1, x_ref, rows_of(near, t_loc), dev_x),
             x_copy(2, x_ref, rows_of(far, t_loc), peer)]
    nx = ep_x * t_loc
    from_x = [x_copy(4, rows_of(nx, h_loc), rows_of(half + nx, h_loc), peer),
              x_copy(3, rows_of(nx, t_loc), rows_of(nx, t_loc), dev_c)]
    from_y = [x_copy(5, rows_of(far + h_loc, h_loc), rows_of(far + h_loc, h_loc), dev_x),
              x_copy(6, rows_of(far, t_loc), rows_of(far, t_loc), dev_c)]
    from_d = [x_copy(7, rows_of(half + nx, t_loc), rows_of(half + nx, t_loc), dev_c)]

    for kind in range(2):
        for dt, de in others:
            gather(kind, dt, de).start()
    for c in x_own:
        c.start()
    r_all[ep] = route_ref[...]
    g_all[ep] = gates_ref[...]
    x_all[pl.ds(pl.multiple_of(near, t_loc), t_loc), :] = x_ref[...]
    for kind in range(2):
        for dt, de in others:
            gather(kind, dt, de).wait()

    route = jnp.concatenate([r_all[i] for i in range(8)], axis=1)
    gates = jnp.concatenate([g_all[i] for i in range(4)], axis=1)
    n_all = 4 * n_e
    e_all = iota((n_all, n_tok), 0)
    e_loc = iota((n_e, n_tok), 0) + ep * n_e
    hit_all = jnp.zeros((n_all, n_tok), F32)
    hit = jnp.zeros((n_e, n_tok), F32)
    gate = jnp.zeros((n_e, half), F32)
    for k in range(route.shape[0]):
        row = route[k:k + 1, :]
        hit_all = jnp.where(row == e_all, 1.0, hit_all)
        same = row == e_loc
        hit = jnp.where(same, 1.0, hit)
        gate = jnp.where(same[:, :half], gates[k:k + 1, :], gate)
    u2, s2 = iota((n_tok, 128), 0), iota((n_tok, 128), 1)
    side = jnp.where((s2 == 0) & (u2 < half) | (s2 == 1) & (u2 >= half), 1.0, 0.0).astype(BF16)
    k_i, s_i = iota((n_all, n_all), 0), iota((n_all, n_all), 1)
    in_block = functools.reduce(lambda a, c: a | c, [(k_i >= i * n_e) & (k_i < (i + 1) * n_e) & (s_i >= i * n_e) & (s_i < (i + 1) * n_e) for i in range(4)])
    suffix = jnp.where((s_i >= k_i) & in_block, 1.0, 0.0).astype(BF16)
    left = dot(suffix, (dot(hit_all.astype(BF16), side) - b).astype(BF16))
    need_ref[0, 0] = jnp.where(jnp.max(left) > flush, 1, 0)

    hit_b = hit.astype(BF16)
    pos = dot(hit_b, before[...])
    code[...] = jnp.where(hit > 0, pos + jnp.where(iota((n_e, n_tok), 1) >= half, float(half // 2), 0.0), -1.0)
    upto = jnp.where(iota((n_e, n_e), 1) <= iota((n_e, n_e), 0), 1.0, 0.0).astype(BF16)
    cum = dot(upto, dot(hit_b, side).astype(BF16))

    k_f = iota((n_e, n_rows), 0).astype(F32)
    i_f = iota((1, n_rows), 1).astype(F32)
    if b:
        step = jnp.minimum(jnp.floor((i_f + 0.5) * (1.0 / b)), float(n_e))
    else:
        step = jnp.full((1, n_rows), float(n_e), F32)
    off = i_f - step * b

    def table(c, shift):
        total = jnp.max(c, axis=0, keepdims=True)

        def served(m):
            inner = jnp.min(jnp.where(k_f <= m, c + b * (m - k_f), BIG), axis=0, keepdims=True)
            return jnp.minimum(inner, b * (m + 1.0))

        q = served(step - 1.0) + off + base_ref[0].astype(F32)
        end = jnp.where(step < n_e, served(step), total)
        valid = q < end
        past = c <= q
        expert = jnp.sum(jnp.where(past, 1.0, 0.0), axis=0, keepdims=True)
        rank = q - jnp.max(jnp.where(past, c, 0.0), axis=0, keepdims=True)
        idx = jnp.where(valid, expert * half + rank + shift, 0.0)
        return idx.astype(jnp.int32), expert, rank, valid

    idx_b, _, _, _ = table(cum[:, 1:2], float(half // 2))
    idx_a, expert, rank, valid = table(cum[:, 0:1], 0.0)
    r8 = iota((8, n_rows), 0)
    tab_v[...] = jnp.where(r8 == 0, idx_b, idx_a)
    to_smem = pltpu.make_async_copy(tab_v, tab_s, tab_sem)
    to_smem.start()

    for i in (1, 2):
        x_own[i].wait_recv()
        for c in (None, from_x, from_y)[i]:
            c.start()

    def columns(a):
        return jnp.transpose(jnp.concatenate([a, jnp.zeros((128 - n_e, half), F32)], axis=0))

    one = jnp.where((iota((128, n_rows), 0).astype(F32) == expert) & valid, 1.0, 0.0).astype(BF16)
    same = dot(columns(pos[:, :half]).astype(BF16), one) == rank
    for j, g in enumerate(split3(columns(gate))):
        full = jnp.where(same, dot(g, one), 0.0).astype(BF16)
        for m in range(n_rows // 128):
            gm[m, j] = full[:, m * 128:(m + 1) * 128]

    from_x[0].wait_recv()
    from_y[0].wait_recv()
    from_d[0].start()
    to_smem.wait()
    x_own[0].wait_recv()
    from_x[1].wait_recv()
    from_y[1].wait_recv()
    from_d[0].wait_recv()

    def chunk(e):
        slot = lax.rem(e, ring)
        return pltpu.make_async_remote_copy(
            src_ref=send.at[slot], dst_ref=recv.at[pl.ds(pl.multiple_of(e * b, b), b)], send_sem=s_sem.at[slot],
            recv_sem=r_sem.at[e], device_id=peer, device_id_type=MESH)

    def piece(f):
        return pltpu.make_async_remote_copy(
            src_ref=fsend.at[pl.ds(pl.multiple_of(f * fb, fb), fb)],
            dst_ref=recv.at[pl.ds(pl.multiple_of(n_main + f * fb, fb), fb)], send_sem=fs_sem.at[f],
            recv_sem=fr_sem.at[f], device_id=peer, device_id_type=MESH)

    def col_piece(n):
        cols = pl.ds(n * wide, wide)
        return pltpu.make_async_remote_copy(
            src_ref=fsend.at[pl.ds(rows_part, cols_part), cols],
            dst_ref=recv.at[pl.ds(n_main + rows_part, cols_part), cols], send_sem=cs_sem.at[n],
            recv_sem=cr_sem.at[n], device_id=peer, device_id_type=MESH)

    def partial(way, i):
        return o_buf[pl.ds(jnp.clip(tab_s[way, i], 0, n_e * half - 1), 1), :]

    def pack_send(e):
        s = lax.rem(e, ring)
        for r in range(b):
            send[s, r:r + 1, :] = partial(0, e * b + r)

    def pack_own(e):
        first = pl.multiple_of(lax.rem(e * b, 128), b)
        for r in range(b):
            own[pl.ds(first + r, 1), :] = partial(1, e * b + r)

    def combine(m, cols):
        o = (recv[m * 128:(m + 1) * 128, cols] + own[:, cols]).astype(BF16)
        y_acc[:, cols] += dot(gm[m, 0], o) + dot(gm[m, 1], o) + dot(gm[m, 2], o)

    def combine_main(m):
        @pl.loop(m * (128 // b), (m + 1) * (128 // b))
        def _(e):
            chunk(e).wait_recv()
        combine(m, slice(None))

    slot_i = iota((half, n_tok), 0).astype(F32)

    @pl.loop(0, n_e)
    def _(e):
        slot = lax.rem(e, depth)
        if b:
            @pl.when(e > ring)
            def _():
                chunk(e - 1 - ring).wait_send()
        for c in weights(e, slot):
            c.wait()
        if b:
            pack_send(jnp.maximum(e - 1, 0))
            pack_own(jnp.maximum(e - lag, 0))
        pick = jnp.where(code[pl.ds(e, 1), :] == slot_i, 1.0, 0.0).astype(BF16)
        xs = dot(pick, x_all[...]).astype(BF16)
        u = dot(xs, w1b[slot])
        v = dot(xs, w3b[slot])
        h = (u * jax.nn.sigmoid(u) * v).astype(BF16)
        o_buf[pl.ds(pl.multiple_of(e * half, half), half), :] = dot(h, w2b[slot])
        if b:
            @pl.when(e >= 1)
            def _():
                chunk(e - 1).start()

        @pl.when(e + depth < n_e)
        def _():
            for c in weights(e + depth, slot):
                c.start()

        if b:
            for m in range(n_main // 128 - 1):
                @pl.when(e == (m + 1) * 128 // b - 1 + lag)
                def _():
                    combine_main(m)

    if b:
        chunk(n_e - 1 - ring).wait_send()
        pack_send(n_e - 1)
        chunk(n_e - 1).start()

    @pl.loop(0, rows_part // fb)
    def _(f):
        for r in range(fb):
            fsend[pl.ds(pl.multiple_of(f * fb, fb) + r, 1), :] = partial(0, n_main + f * fb + r)
        piece(f).start()

    @pl.loop(0, cols_part // 8)
    def _(f):
        for r in range(8):
            i = rows_part + f * 8 + r
            fsend[pl.ds(i, 1), :] = partial(0, n_main + i)
    for n in range(nb):
        col_piece(n).start()

    if b:
        @pl.loop(n_e - lag, n_e)
        def _(e):
            pack_own(e)
        combine_main(n_main // 128 - 1)

        @pl.loop(n_e - ring, n_e)
        def _(e):
            chunk(e).wait_send()

    def give(o, n):
        to = lax.rem(ep + o, 4)
        cols = pl.ds(n * wide, wide)
        return pltpu.make_async_remote_copy(
            src_ref=y_acc.at[pl.ds(pl.multiple_of(to * t_loc, t_loc), t_loc), cols], dst_ref=y_recv.at[3 - o, :, cols],
            send_sem=ys_sem.at[o - 1, n], recv_sem=yr_sem.at[3 - o, n], device_id={"tp": tp, "ep": to}, device_id_type=MESH)

    last = n_rows // 128 - 1
    for m in range(n_main // 128, last + 1):
        @pl.loop(0, 16)
        def _(f):
            for r in range(8):
                own[pl.ds(pl.multiple_of(f * 8, 8) + r, 1), :] = partial(1, m * 128 + f * 8 + r)
        if m < last:
            for f in range(128 // fb):
                piece((m * 128 - n_main) // fb + f).wait_recv()
            combine(m, slice(None))
    for f in range((last * 128 - n_main) // fb, rows_part // fb):
        piece(f).wait_recv()
    for n in range(nb):
        col_piece(n).wait_recv()
        combine(last, slice(n * wide, (n + 1) * wide))
        for o in (2, 1, 3):
            give(o, n).start()
    mine = pl.ds(pl.multiple_of(near, t_loc), t_loc)
    for n in range(nb):
        cols = slice(n * wide, (n + 1) * wide)
        y = y_acc[mine, cols]
        for o in (1, 3, 2):
            give(o, n).wait_recv()
            y = y + y_recv[3 - o, :, cols]
        y_ref[:, cols] = y.astype(y_ref.dtype)

    for f in range(rows_part // fb):
        piece(f).wait_send()
    for n in range(nb):
        col_piece(n).wait_send()
        for o in (1, 2, 3):
            give(o, n).wait_send()
    for c in x_own + from_x + from_y + from_d:
        c.wait_send()


def moe_call(b, rows_part, cols_part, fb, nb, depth, ring, out_dtype, cid, base, x, route, gates, w1, w3, w2):
    t_loc, d = x.shape
    n_e, _, f = w1.shape
    n_rows = n_e * b + rows_part + cols_part
    half = 4 * t_loc
    dma = pltpu.SemaphoreType.DMA
    vm = pl.BlockSpec(memory_space=pltpu.VMEM)
    sm = pl.BlockSpec(memory_space=pltpu.SMEM)
    hbm = pl.BlockSpec(memory_space=pl.ANY)
    return pl.pallas_call(
        functools.partial(moe_kernel, b, rows_part, cols_part, fb, nb, depth, ring),
        out_shape=(jax.ShapeDtypeStruct((t_loc, d), out_dtype), jax.ShapeDtypeStruct((1, 1), jnp.int32)),
        in_specs=[sm, vm, vm, vm, hbm, hbm, hbm],
        out_specs=(vm, sm),
        scratch_shapes=[
            pltpu.VMEM((2 * half, d), BF16),
            pltpu.VMEM((8,) + route.shape, jnp.int32),
            pltpu.VMEM((8,) + route.shape, F32),
            pltpu.VMEM((2 * half, 2 * half), BF16),
            pltpu.VMEM((n_e, 2 * half), F32),
            pltpu.VMEM((n_rows // 128, 3, half, 128), BF16),
            pltpu.VMEM((8, n_rows), jnp.int32),
            pltpu.SMEM((8, n_rows), jnp.int32),
            pltpu.VMEM((depth, d, f), BF16),
            pltpu.VMEM((depth, d, f), BF16),
            pltpu.VMEM((depth, f, d), BF16),
            pltpu.VMEM((n_e * half, d), F32),
            pltpu.VMEM((ring, max(b, 8), d), F32),
            pltpu.VMEM((rows_part + cols_part, d), F32),
            pltpu.VMEM((n_rows, d), F32),
            pltpu.VMEM((128, d), F32),
            pltpu.VMEM((half, d), F32),
            pltpu.VMEM((3, t_loc, d), F32),
            dma((2, 8)), dma((2, 8)), dma((8,)), dma((8,)), dma, dma((3, depth)), dma((ring,)), dma((n_e,)),
            dma((rows_part // fb,)), dma((rows_part // fb,)), dma((nb,)), dma((nb,)), dma((3, nb)), dma((3, nb)),
        ],
        compiler_params=pltpu.CompilerParams(collective_id=cid, has_side_effects=True, vmem_limit_bytes=67043328),
    )(base, x, route, gates, w1, w3, w2)


def solution(mesh):
    tok_spec = P(('dp', 'tp', 'ep'), None)

    def local(x, route_idx, gates, w1, w3, w2):
        zero = jnp.zeros((1,), jnp.int32)
        rt, gt = route_idx.T, gates.T
        y, need = moe_call(8, 64, 64, 16, 4, 3, 4, BF16, 1, zero, x, rt, gt, w1, w3, w2)

        def slow(_):
            part = 256

            def one(p, acc):
                base = jnp.full((1,), p * part, jnp.int32)
                return acc + moe_call(0, part - 64, 64, 16, 4, 3, 4, F32, 2, base, x, rt, gt, w1, w3, w2)[0]

            return lax.fori_loop(0, 1024 // part, one, jnp.zeros(x.shape, F32)).astype(BF16)

        return lax.cond(need[0, 0] > 0, slow, lambda y: y, y)

    return jax.shard_map(local, mesh=mesh,
                         in_specs=(tok_spec, tok_spec, tok_spec, P('ep', None, 'tp'), P('ep', None, 'tp'), P('ep', 'tp', None)),
                         out_specs=tok_spec, check_vma=False)
```

```python
import functools

import jax
import jax.numpy as jnp
from jax import lax
from jax.experimental import pallas as pl
from jax.experimental.pallas import tpu as pltpu
from jax.sharding import PartitionSpec as P

MESH = pl.DeviceIdType.MESH
F32 = jnp.float32
BF16 = jnp.bfloat16
BIG = 1e9


def dot(a, b):
    return jnp.dot(a, b, preferred_element_type=F32)


def iota(shape, dim):
    return lax.broadcasted_iota(jnp.int32, shape, dim)


def split3(g):
    g1 = g.astype(BF16)
    r = g - g1.astype(F32)
    g2 = r.astype(BF16)
    g3 = (r - g2.astype(F32)).astype(BF16)
    return g1, g2, g3


def moe_kernel(b, rows_part, cols_part, fb, nb, depth, ring, *refs):
    (base_ref, x_ref, route_ref, gates_ref, w1_ref, w3_ref, w2_ref, y_ref, need_ref,
     x_all, r_all, g_all, before, code, gm, gf, tab_v, tab_s, w1b, w3b, w2b, o_buf, send, recv, own, y_acc, y_recv,
     cand, swap, f_send, f_recv,
     gs_sem, gr_sem, xs_sem, xr_sem, tab_sem, w_sem, s_sem, r_sem, ds_sem, dr_sem, fs_sem, fr_sem, cs_sem, cr_sem,
     ys_sem, yr_sem) = refs
    tp = lax.axis_index("tp")
    ep = lax.axis_index("ep")
    t_loc, d = x_ref.shape
    n_e = w1_ref.shape[0]
    half = 4 * t_loc
    n_tok = 2 * half
    flush = rows_part + cols_part
    n_main = n_e * b
    lag = 4
    hw = d // 2
    wide = hw // nb
    core = lax.rem(ep, 2)
    tp_peer = lax.rem(tp + 1, 2)
    ep_x = lax.rem(ep + 2, 4)
    ep_c = ep + 1 - 2 * lax.rem(ep, 2)
    ep_d = lax.rem(ep_c + 2, 4)
    peer = {"tp": tp_peer, "ep": ep}
    dev_x = {"tp": tp, "ep": ep_x}
    dev_c = {"tp": tp, "ep": ep_c}

    def weights(e, slot):
        return [pltpu.make_async_copy(w1_ref.at[e], w1b.at[slot], w_sem.at[0, slot]),
                pltpu.make_async_copy(w3_ref.at[e], w3b.at[slot], w_sem.at[1, slot]),
                pltpu.make_async_copy(w2_ref.at[e], w2b.at[slot], w_sem.at[2, slot])]

    for e in range(depth):
        for c in weights(e, e):
            c.start()

    others = [(dt, de) for dt in range(2) for de in range(4) if (dt, de) != (0, 0)]

    def device(dt, de):
        return {"tp": lax.rem(tp + dt, 2), "ep": lax.rem(ep + de, 4)}

    barrier = pltpu.get_barrier_semaphore()
    for dt, de in others:
        pl.semaphore_signal(barrier, inc=1, device_id=device(dt, de), device_id_type=MESH)

    t_i, u_i = iota((n_tok, n_tok), 0), iota((n_tok, n_tok), 1)
    before[...] = jnp.where((t_i < u_i) & ((t_i < half) == (u_i < half)), 1.0, 0.0).astype(BF16)
    y_acc[...] = jnp.zeros_like(y_acc)
    o_buf[n_e * half:, :] = jnp.zeros((8, d), F32)
    pl.semaphore_wait(barrier, len(others))

    def gather(kind, dt, de):
        src, dst = ((route_ref, r_all), (gates_ref, g_all))[kind]
        return pltpu.make_async_remote_copy(
            src_ref=src, dst_ref=dst.at[dt * 4 + ep], send_sem=gs_sem.at[kind, dt * 4 + de],
            recv_sem=gr_sem.at[kind, dt * 4 + de], device_id=device(dt, de), device_id_type=MESH)

    def rows_of(first, n):
        return x_all.at[pl.ds(pl.multiple_of(first, 16), n)]

    def x_copy(i, src, dst, to):
        return pltpu.make_async_remote_copy(src_ref=src, dst_ref=dst, send_sem=xs_sem.at[i], recv_sem=xr_sem.at[i],
                                            device_id=to, device_id_type=MESH)

    near, far, h_loc = ep * t_loc, half + ep * t_loc, t_loc // 2
    nx = ep_x * t_loc
    x_own = [x_copy(0, x_ref.at[pl.ds(0, h_loc)], rows_of(near, h_loc), dev_x),
             x_copy(1, x_ref.at[pl.ds(h_loc, h_loc)], rows_of(far + h_loc, h_loc), peer),
             x_copy(2, x_ref.at[pl.ds(h_loc, h_loc)], rows_of(near + h_loc, h_loc), dev_x),
             x_copy(3, x_ref.at[pl.ds(0, h_loc)], rows_of(far, h_loc), peer),
             x_copy(4, x_ref, rows_of(near, t_loc), dev_c)]

    def passed(i, row, n, to):
        return x_copy(i, rows_of(row, n), rows_of(row, n), to)

    to_y = x_copy(5, rows_of(nx, h_loc), rows_of(half + nx, h_loc), peer)
    to_x = passed(6, far + h_loc, h_loc, dev_x)
    to_c = [passed(7, nx, t_loc, dev_c), passed(8, far, t_loc, dev_c),
            passed(9, half + nx, h_loc, dev_c), passed(10, half + nx + h_loc, h_loc, dev_c)]

    for kind in range(2):
        for dt, de in others:
            gather(kind, dt, de).start()
    for c in x_own:
        c.start()
    r_all[ep] = route_ref[...]
    g_all[ep] = gates_ref[...]
    x_all[pl.ds(pl.multiple_of(near, t_loc), t_loc), :] = x_ref[...]
    for kind in range(2):
        for dt, de in others:
            gather(kind, dt, de).wait()

    route = jnp.concatenate([r_all[i] for i in range(8)], axis=1)
    gates = jnp.concatenate([g_all[i] for i in range(4)], axis=1)
    n_all = 4 * n_e
    e_all = iota((n_all, n_tok), 0)
    e_two = iota((2 * n_e, n_tok), 0)
    e_two = jnp.where(e_two < n_e, e_two + ep * n_e, e_two + (ep_c - 1) * n_e)
    hit_all = jnp.zeros((n_all, n_tok), F32)
    hit = jnp.zeros((2 * n_e, n_tok), F32)
    gate = jnp.zeros((2 * n_e, half), F32)
    for k in range(route.shape[0]):
        row = route[k:k + 1, :]
        hit_all = jnp.where(row == e_all, 1.0, hit_all)
        same = row == e_two
        hit = jnp.where(same, 1.0, hit)
        gate = jnp.where(same[:, :half], gates[k:k + 1, :], gate)
    u2, s2 = iota((n_tok, 128), 0), iota((n_tok, 128), 1)
    side = jnp.where((s2 == 0) & (u2 < half) | (s2 == 1) & (u2 >= half), 1.0, 0.0).astype(BF16)
    k_i, s_i = iota((n_all, n_all), 0), iota((n_all, n_all), 1)
    in_block = functools.reduce(lambda a, c: a | c, [(k_i >= i * n_e) & (k_i < (i + 1) * n_e) & (s_i >= i * n_e) & (s_i < (i + 1) * n_e) for i in range(4)])
    suffix = jnp.where((s_i >= k_i) & in_block, 1.0, 0.0).astype(BF16)
    left = dot(suffix, (dot(hit_all.astype(BF16), side) - b).astype(BF16))
    left = [jnp.maximum(jnp.max(left[i * n_e:(i + 1) * n_e], axis=0, keepdims=True), 0.0) for i in range(4)]
    need_ref[0, 0] = jnp.where(jnp.max(jnp.maximum(left[0] + left[1], left[2] + left[3])) > flush, 1, 0)

    hit_b = hit.astype(BF16)
    pos = dot(hit_b, before[...])
    code[...] = jnp.where(hit > 0, pos + jnp.where(iota((2 * n_e, n_tok), 1) >= half, float(half // 2), 0.0), -1.0)[:n_e]
    two = 2 * n_e
    up_i, up_j = iota((two, two), 0), iota((two, two), 1)
    upto = jnp.where((up_j <= up_i) & ((up_j < n_e) == (up_i < n_e)), 1.0, 0.0).astype(BF16)
    cum = dot(upto, dot(hit_b, side).astype(BF16))

    def served(c, m, k_f):
        inner = jnp.min(jnp.where(k_f <= m, c + b * (m - k_f), BIG), axis=0, keepdims=True)
        return jnp.minimum(inner, b * (m + 1.0))

    def locate(c, q, valid, shift):
        past = c <= q
        expert = jnp.sum(jnp.where(past, 1.0, 0.0), axis=0, keepdims=True)
        rank = q - jnp.max(jnp.where(past, c, 0.0), axis=0, keepdims=True)
        idx = jnp.where(valid, expert * half + rank + shift, float(n_e * half))
        return idx.astype(jnp.int32), expert, rank

    def main_table(way, shift):
        c = cum[:n_e, way:way + 1]
        k_f = iota((n_e, n_main), 0).astype(F32)
        i_f = iota((1, n_main), 1).astype(F32)
        step = jnp.floor((i_f + 0.5) * (1.0 / b))
        q = served(c, step - 1.0, k_f) + (i_f - step * b)
        valid = q < served(c, step, k_f)
        return locate(c, q, valid, shift) + (valid,)

    def flush_table(way, shift):
        k_f = iota((n_e, 256), 0).astype(F32)
        i_f = iota((1, 256), 1).astype(F32) + base_ref[0].astype(F32)
        both = []
        for c in (cum[:n_e, way:way + 1], cum[n_e:, way:way + 1]):
            done = served(c, float(n_e - 1), k_f)
            both.append((c, done, jnp.max(c, axis=0, keepdims=True) - done))
        second = core.astype(F32)
        out = []
        for (c, done, rest), first in zip(both, (second * both[1][2], (1.0 - second) * both[0][2])):
            i = i_f - first
            valid = (i >= 0) & (i < rest)
            out.append(locate(c, done + i, valid, shift) + (valid,))
        return out

    def one_hot(expert, valid, n):
        return jnp.where((iota((n, expert.shape[1]), 0).astype(F32) == expert) & valid, 1.0, 0.0)

    b_own, _ = flush_table(1, float(half // 2))
    a_own, a_par = flush_table(0, 0.0)
    picks = [(b_own[0], a_own[0], jnp.concatenate([one_hot(a_own[1], a_own[3], n_e), one_hot(a_par[1], a_par[3], n_e),
                                                   jnp.zeros((128 - two, 256), F32)], axis=0),
              jnp.where(a_own[3], a_own[2], a_par[2]))]
    if b:
        m_b, m_a = main_table(1, float(half // 2)), main_table(0, 0.0)
        picks.insert(0, (m_b[0], m_a[0], one_hot(m_a[1], m_a[3], 128), m_a[2]))
    idx_b, idx_a, one, rank = [jnp.concatenate(p, axis=1) for p in zip(*picks)]
    tab_v[...] = jnp.where(iota(tab_v.shape, 0) == 0, idx_b, idx_a)
    to_smem = pltpu.make_async_copy(tab_v, tab_s, tab_sem)
    to_smem.start()

    x_own[0].wait_recv()
    to_y.start()
    x_own[1].wait_recv()
    to_x.start()
    x_own[2].wait_recv()
    to_c[0].start()
    x_own[3].wait_recv()
    to_c[1].start()

    def columns(a):
        return jnp.transpose(jnp.concatenate([a, jnp.zeros((128 - two, half), F32)], axis=0))

    one = one.astype(BF16)
    same = dot(columns(pos[:, :half]).astype(BF16), one) == rank
    for j, g in enumerate(split3(columns(gate))):
        full = jnp.where(same, dot(g, one), 0.0).astype(BF16)
        for m in range(n_main // 128):
            gm[m, j] = full[:, m * 128:(m + 1) * 128]
        gf[j] = full[:, n_main:]

    to_y.wait_recv()
    to_c[2].start()
    to_x.wait_recv()
    to_c[3].start()
    to_smem.wait()
    x_own[4].wait_recv()
    for c in to_c:
        c.wait_recv()

    def chunk(e):
        slot = lax.rem(e, ring)
        return pltpu.make_async_remote_copy(
            src_ref=send.at[slot], dst_ref=recv.at[pl.ds(pl.multiple_of(e * b, b), b)], send_sem=s_sem.at[slot],
            recv_sem=r_sem.at[e], device_id=peer, device_id_type=MESH)

    def swapped(way, f):
        rows = pl.ds(f * fb, fb) if f < rows_part // fb else pl.ds(rows_part, cols_part)
        return pltpu.make_async_remote_copy(
            src_ref=cand.at[way, 1 - core, rows], dst_ref=swap.at[way, rows], send_sem=ds_sem.at[way, f],
            recv_sem=dr_sem.at[way, f], device_id=dev_c, device_id_type=MESH)

    def piece(f):
        rows = pl.ds(f * fb, fb)
        return pltpu.make_async_remote_copy(src_ref=f_send.at[rows], dst_ref=f_recv.at[rows], send_sem=fs_sem.at[f],
                                            recv_sem=fr_sem.at[f], device_id=peer, device_id_type=MESH)

    def col_piece(n):
        at = (pl.ds(rows_part, cols_part), pl.ds(n * wide, wide))
        return pltpu.make_async_remote_copy(src_ref=f_send.at[at], dst_ref=f_recv.at[at], send_sem=cs_sem.at[n],
                                            recv_sem=cr_sem.at[n], device_id=peer, device_id_type=MESH)

    def partial(way, i):
        return o_buf[pl.ds(jnp.clip(tab_s[way, i], 0, n_e * half), 1), :]

    def pack_send(e):
        s = lax.rem(e, ring)
        for r in range(b):
            send[s, r:r + 1, :] = partial(0, e * b + r)

    def pack_own(e):
        first = pl.multiple_of(lax.rem(e * b, 128), b)
        for r in range(b):
            own[pl.ds(first + r, 1), :] = partial(1, e * b + r)

    def combine_main(m):
        @pl.loop(m * (128 // b), (m + 1) * (128 // b))
        def _(e):
            chunk(e).wait_recv()
        for h in range(2):
            cols = slice(h * hw, (h + 1) * hw)
            o = (recv[m * 128:(m + 1) * 128, cols] + own[:, cols]).astype(BF16)
            y_acc[h] += dot(gm[m, 0], o) + dot(gm[m, 1], o) + dot(gm[m, 2], o)

    def combine_flush(rows, cols):
        o = (f_recv[rows, cols] + (cand[0, core, rows, cols] + swap[0, rows, cols])).astype(BF16)
        y_acc[core, :, cols] += dot(gf[0, :, rows], o) + dot(gf[1, :, rows], o) + dot(gf[2, :, rows], o)

    slot_i = iota((half, n_tok), 0).astype(F32)

    @pl.loop(0, n_e)
    def _(e):
        slot = lax.rem(e, depth)
        if b:
            @pl.when(e > ring)
            def _():
                chunk(e - 1 - ring).wait_send()

            @pl.when(e >= 1)
            def _():
                pack_send(e - 1)
                chunk(e - 1).start()
        for c in weights(e, slot):
            c.wait()
        if b:
            pack_own(jnp.maximum(e - lag, 0))
        pick = jnp.where(code[pl.ds(e, 1), :] == slot_i, 1.0, 0.0).astype(BF16)
        xs = dot(pick, x_all[...]).astype(BF16)
        u = dot(xs, w1b[slot])
        v = dot(xs, w3b[slot])
        h = (u * jax.nn.sigmoid(u) * v).astype(BF16)
        o_buf[pl.ds(pl.multiple_of(e * half, half), half), :] = dot(h, w2b[slot])

        @pl.when(e + depth < n_e)
        def _():
            for c in weights(e + depth, slot):
                c.start()

        if b:
            for m in range(n_main // 128 - 1):
                @pl.when(e == (m + 1) * 128 // b - 1 + lag)
                def _():
                    combine_main(m)

    if b:
        chunk(n_e - 1 - ring).wait_send()
        pack_send(n_e - 1)
        chunk(n_e - 1).start()

    n_piece = rows_part // fb + 1

    def pack_cand(way, f):
        first, n = (f * fb, fb) if f < n_piece - 1 else (rows_part, cols_part)

        @pl.loop(0, n // 8)
        def _(g):
            for r in range(8):
                i = first + g * 8 + r
                row = partial(1 - way, n_main + i)
                cand[way, 0, pl.ds(i, 1), :] = row[:, :hw]
                cand[way, 1, pl.ds(i, 1), :] = row[:, hw:]
        swapped(way, f).start()

    def join_send(f):
        swapped(1, f).wait_recv()
        rows = slice(f * fb, (f + 1) * fb) if f < n_piece - 1 else slice(rows_part, flush)
        f_send[rows, :] = cand[1, core, rows, :] + swap[1, rows, :]
        if f < n_piece - 1:
            piece(f).start()
        else:
            for n in range(nb):
                col_piece(n).start()

    def give(o, n):
        to = lax.rem(ep + o, 4)
        h, cols = (core, pl.ds(n * wide, wide)) if n < nb else (1 - core, pl.ds(0, hw))
        return pltpu.make_async_remote_copy(
            src_ref=y_acc.at[h, pl.ds(pl.multiple_of(to * t_loc, t_loc), t_loc), cols], dst_ref=y_recv.at[3 - o, h, :, cols],
            send_sem=ys_sem.at[o - 1, n], recv_sem=yr_sem.at[3 - o, n], device_id={"tp": tp, "ep": to}, device_id_type=MESH)

    for f in range(2):
        pack_cand(1, f)
    for f in range(n_piece):
        join_send(f)
        if f + 2 < n_piece:
            pack_cand(1, f + 2)
    if b:
        @pl.loop(n_e - lag, n_e)
        def _(e):
            pack_own(e)
        combine_main(n_main // 128 - 1)
    for o in (2, 1, 3):
        give(o, nb).start()
    for f in range(n_piece):
        pack_cand(0, f)
    for f in range(n_piece):
        swapped(0, f).wait_recv()
    for f in range(n_piece - 1):
        piece(f).wait_recv()
    combine_flush(slice(0, rows_part), slice(0, hw))
    for n in range(nb):
        col_piece(n).wait_recv()
        combine_flush(slice(rows_part, flush), slice(n * wide, (n + 1) * wide))
        for o in (2, 1, 3):
            give(o, n).start()
    for n in (nb,) + tuple(range(nb)):
        for o in (1, 3, 2):
            give(o, n).wait_recv()
    mine = pl.ds(pl.multiple_of(near, t_loc), t_loc)
    for h in range(2):
        y = y_acc[h, mine, :]
        for o in (1, 3, 2):
            y = y + y_recv[3 - o, h]
        y_ref[:, h * hw:(h + 1) * hw] = y.astype(y_ref.dtype)

    if b:
        @pl.loop(n_e - ring, n_e)
        def _(e):
            chunk(e).wait_send()
    for f in range(n_piece):
        for way in range(2):
            swapped(way, f).wait_send()
        if f < n_piece - 1:
            piece(f).wait_send()
    for n in range(nb + 1):
        if n < nb:
            col_piece(n).wait_send()
        for o in (1, 2, 3):
            give(o, n).wait_send()
    for c in x_own + [to_y, to_x] + to_c:
        c.wait_send()


def moe_call(b, rows_part, cols_part, fb, nb, depth, ring, out_dtype, cid, base, x, route, gates, w1, w3, w2):
    t_loc, d = x.shape
    n_e, _, f = w1.shape
    n_main = n_e * b
    flush = rows_part + cols_part
    half = 4 * t_loc
    n_piece = rows_part // fb
    dma = pltpu.SemaphoreType.DMA
    vm = pl.BlockSpec(memory_space=pltpu.VMEM)
    sm = pl.BlockSpec(memory_space=pltpu.SMEM)
    hbm = pl.BlockSpec(memory_space=pl.ANY)
    return pl.pallas_call(
        functools.partial(moe_kernel, b, rows_part, cols_part, fb, nb, depth, ring),
        out_shape=(jax.ShapeDtypeStruct((t_loc, d), out_dtype), jax.ShapeDtypeStruct((1, 1), jnp.int32)),
        in_specs=[sm, vm, vm, vm, hbm, hbm, hbm],
        out_specs=(vm, sm),
        scratch_shapes=[
            pltpu.VMEM((2 * half, d), BF16),
            pltpu.VMEM((8,) + route.shape, jnp.int32),
            pltpu.VMEM((8,) + route.shape, F32),
            pltpu.VMEM((2 * half, 2 * half), BF16),
            pltpu.VMEM((n_e, 2 * half), F32),
            pltpu.VMEM((max(n_main // 128, 1), 3, half, 128), BF16),
            pltpu.VMEM((3, half, 256), BF16),
            pltpu.VMEM((8, n_main + 256), jnp.int32),
            pltpu.SMEM((8, n_main + 256), jnp.int32),
            pltpu.VMEM((depth, d, f), BF16),
            pltpu.VMEM((depth, d, f), BF16),
            pltpu.VMEM((depth, f, d), BF16),
            pltpu.VMEM((n_e * half + 8, d), F32),
            pltpu.VMEM((ring, max(b, 8), d), F32),
            pltpu.VMEM((max(n_main, 8), d), F32),
            pltpu.VMEM((128, d), F32),
            pltpu.VMEM((2, half, d // 2), F32),
            pltpu.VMEM((3, 2, t_loc, d // 2), F32),
            pltpu.VMEM((2, 2, flush, d // 2), F32),
            pltpu.VMEM((2, flush, d // 2), F32),
            pltpu.VMEM((flush, d // 2), F32),
            pltpu.VMEM((flush, d // 2), F32),
            dma((2, 8)), dma((2, 8)), dma((11,)), dma((11,)), dma, dma((3, depth)), dma((ring,)), dma((n_e,)),
            dma((2, n_piece + 1)), dma((2, n_piece + 1)), dma((n_piece,)), dma((n_piece,)), dma((nb,)), dma((nb,)),
            dma((3, nb + 1)), dma((3, nb + 1)),
        ],
        compiler_params=pltpu.CompilerParams(collective_id=cid, has_side_effects=True, vmem_limit_bytes=67043328),
    )(base, x, route, gates, w1, w3, w2)


def solution(mesh):
    tok_spec = P(('dp', 'tp', 'ep'), None)

    def local(x, route_idx, gates, w1, w3, w2):
        zero = jnp.zeros((1,), jnp.int32)
        rt, gt = route_idx.T, gates.T
        y, need = moe_call(8, 128, 64, 32, 4, 3, 4, BF16, 1, zero, x, rt, gt, w1, w3, w2)

        def slow(_):
            part = 192

            def one(p, acc):
                base = jnp.full((1,), p * part, jnp.int32)
                return acc + moe_call(0, 128, part - 128, 32, 4, 3, 4, F32, 2, base, x, rt, gt, w1, w3, w2)[0]

            return lax.fori_loop(0, pl.cdiv(2048, part), one, jnp.zeros(x.shape, F32)).astype(BF16)

        return lax.cond(need[0, 0] > 0, slow, lambda y: y, y)

    return jax.shard_map(local, mesh=mesh,
                         in_specs=(tok_spec, tok_spec, tok_spec, P('ep', None, 'tp'), P('ep', None, 'tp'), P('ep', 'tp', None)),
                         out_specs=tok_spec, check_vma=False)
```

```python
import functools

import jax
import jax.numpy as jnp
from jax import lax
from jax.experimental import pallas as pl
from jax.experimental.pallas import tpu as pltpu
from jax.sharding import PartitionSpec as P

MESH = pl.DeviceIdType.MESH
F32 = jnp.float32
BF16 = jnp.bfloat16
BIG = 1e9


def dot(a, b):
    return jnp.dot(a, b, preferred_element_type=F32)


def iota(shape, dim):
    return lax.broadcasted_iota(jnp.int32, shape, dim)


def split3(g):
    g1 = g.astype(BF16)
    r = g - g1.astype(F32)
    g2 = r.astype(BF16)
    g3 = (r - g2.astype(F32)).astype(BF16)
    return g1, g2, g3


def moe_kernel(b, rows_part, cols_part, extra, fb, nb, depth, ring, *refs):
    (base_ref, x_ref, route_ref, gates_ref, w1_ref, w3_ref, w2_ref, y_ref, need_ref, mb_ref, ma_ref, mg_ref,
     x_all, r_all, g_all, before, code, gm, gf, tab_v, tab_s, w1b, w3b, w2b, o_buf, send, recv, own, y_acc, y_recv,
     cand, swap, f_send, f_recv,
     gs_sem, gr_sem, xs_sem, xr_sem, tab_sem, w_sem, s_sem, r_sem, ds_sem, dr_sem, fs_sem, fr_sem, cs_sem, cr_sem,
     ys_sem, yr_sem, m_sem) = refs
    tp = lax.axis_index("tp")
    ep = lax.axis_index("ep")
    t_loc, d = x_ref.shape
    n_e = w1_ref.shape[0]
    half = 4 * t_loc
    n_tok = 2 * half
    flush = rows_part + cols_part
    n_main = n_e * b
    lag = 4
    hw = d // 2
    wide = hw // nb
    core = lax.rem(ep, 2)
    tp_peer = lax.rem(tp + 1, 2)
    ep_x = lax.rem(ep + 2, 4)
    ep_c = ep + 1 - 2 * lax.rem(ep, 2)
    ep_d = lax.rem(ep_c + 2, 4)
    peer = {"tp": tp_peer, "ep": ep}
    dev_x = {"tp": tp, "ep": ep_x}
    dev_c = {"tp": tp, "ep": ep_c}

    def weights(e, slot):
        return [pltpu.make_async_copy(w1_ref.at[e], w1b.at[slot], w_sem.at[0, slot]),
                pltpu.make_async_copy(w3_ref.at[e], w3b.at[slot], w_sem.at[1, slot]),
                pltpu.make_async_copy(w2_ref.at[e], w2b.at[slot], w_sem.at[2, slot])]

    for e in range(depth):
        for c in weights(e, e):
            c.start()

    others = [(dt, de) for dt in range(2) for de in range(4) if (dt, de) != (0, 0)]

    def device(dt, de):
        return {"tp": lax.rem(tp + dt, 2), "ep": lax.rem(ep + de, 4)}

    barrier = pltpu.get_barrier_semaphore()
    for dt, de in others:
        pl.semaphore_signal(barrier, inc=1, device_id=device(dt, de), device_id_type=MESH)

    t_i, u_i = iota((n_tok, n_tok), 0), iota((n_tok, n_tok), 1)
    before[...] = jnp.where((t_i < u_i) & ((t_i < half) == (u_i < half)), 1.0, 0.0).astype(BF16)
    y_acc[...] = jnp.zeros_like(y_acc)
    o_buf[n_e * half:, :] = jnp.zeros((8, d), F32)
    pl.semaphore_wait(barrier, len(others))

    def gather(kind, dt, de):
        src, dst = ((route_ref, r_all), (gates_ref, g_all))[kind]
        return pltpu.make_async_remote_copy(
            src_ref=src, dst_ref=dst.at[dt * 4 + ep], send_sem=gs_sem.at[kind, dt * 4 + de],
            recv_sem=gr_sem.at[kind, dt * 4 + de], device_id=device(dt, de), device_id_type=MESH)

    def rows_of(first, n):
        return x_all.at[pl.ds(pl.multiple_of(first, 16), n)]

    def x_copy(i, src, dst, to):
        return pltpu.make_async_remote_copy(src_ref=src, dst_ref=dst, send_sem=xs_sem.at[i], recv_sem=xr_sem.at[i],
                                            device_id=to, device_id_type=MESH)

    near, far, h_loc = ep * t_loc, half + ep * t_loc, t_loc // 2
    nx = ep_x * t_loc
    x_own = [x_copy(0, x_ref.at[pl.ds(0, h_loc)], rows_of(near, h_loc), dev_x),
             x_copy(1, x_ref.at[pl.ds(h_loc, h_loc)], rows_of(far + h_loc, h_loc), peer),
             x_copy(2, x_ref.at[pl.ds(h_loc, h_loc)], rows_of(near + h_loc, h_loc), dev_x),
             x_copy(3, x_ref.at[pl.ds(0, h_loc)], rows_of(far, h_loc), peer),
             x_copy(4, x_ref, rows_of(near, t_loc), dev_c)]

    def passed(i, row, n, to):
        return x_copy(i, rows_of(row, n), rows_of(row, n), to)

    to_y = x_copy(5, rows_of(nx, h_loc), rows_of(half + nx, h_loc), peer)
    to_x = passed(6, far + h_loc, h_loc, dev_x)
    to_c = [passed(7, nx, t_loc, dev_c), passed(8, far, t_loc, dev_c),
            passed(9, half + nx, h_loc, dev_c), passed(10, half + nx + h_loc, h_loc, dev_c)]

    for kind in range(2):
        for dt, de in others:
            gather(kind, dt, de).start()
    for c in x_own:
        c.start()
    r_all[ep] = route_ref[...]
    g_all[ep] = gates_ref[...]
    x_all[pl.ds(pl.multiple_of(near, t_loc), t_loc), :] = x_ref[...]
    for kind in range(2):
        for dt, de in others:
            gather(kind, dt, de).wait()

    x_own[0].wait_recv()
    to_y.start()
    x_own[1].wait_recv()
    to_x.start()

    route = jnp.concatenate([r_all[i] for i in range(8)], axis=1)
    gates = jnp.concatenate([g_all[i] for i in range(4)], axis=1)
    n_all = 4 * n_e
    e_all = iota((n_all, n_tok), 0)
    e_two = iota((2 * n_e, n_tok), 0)
    e_two = jnp.where(e_two < n_e, e_two + ep * n_e, e_two + (ep_c - 1) * n_e)
    hit_all = jnp.zeros((n_all, n_tok), F32)
    hit = jnp.zeros((2 * n_e, n_tok), F32)
    gate = jnp.zeros((2 * n_e, half), F32)
    for k in range(route.shape[0]):
        row = route[k:k + 1, :]
        hit_all = jnp.where(row == e_all, 1.0, hit_all)
        same = row == e_two
        hit = jnp.where(same, 1.0, hit)
        gate = jnp.where(same[:, :half], gates[k:k + 1, :], gate)
    u2, s2 = iota((n_tok, 128), 0), iota((n_tok, 128), 1)
    side = jnp.where((s2 == 0) & (u2 < half) | (s2 == 1) & (u2 >= half), 1.0, 0.0).astype(BF16)
    k_i, s_i = iota((n_all, n_all), 0), iota((n_all, n_all), 1)
    in_block = functools.reduce(lambda a, c: a | c, [(k_i >= i * n_e) & (k_i < (i + 1) * n_e) & (s_i >= i * n_e) & (s_i < (i + 1) * n_e) for i in range(4)])
    suffix = jnp.where((s_i >= k_i) & in_block, 1.0, 0.0).astype(BF16)
    left = dot(suffix, (dot(hit_all.astype(BF16), side) - b).astype(BF16))
    left = [jnp.maximum(jnp.max(left[i * n_e:(i + 1) * n_e], axis=0, keepdims=True), 0.0) for i in range(4)]
    left = jnp.max(jnp.maximum(left[0] + left[1], left[2] + left[3]))
    need_ref[0, 0] = jnp.where(left > flush, 1, 0) + jnp.where(left > flush + extra, 1, 0)

    hit_b = hit.astype(BF16)
    pos = dot(hit_b, before[...])
    code[...] = jnp.where(hit > 0, pos + jnp.where(iota((2 * n_e, n_tok), 1) >= half, float(half // 2), 0.0), -1.0)[:n_e]
    two = 2 * n_e
    up_i, up_j = iota((two, two), 0), iota((two, two), 1)
    upto = jnp.where((up_j <= up_i) & ((up_j < n_e) == (up_i < n_e)), 1.0, 0.0).astype(BF16)
    cum = dot(upto, dot(hit_b, side).astype(BF16))

    def served(c, m, k_f):
        inner = jnp.min(jnp.where(k_f <= m, c + b * (m - k_f), BIG), axis=0, keepdims=True)
        return jnp.minimum(inner, b * (m + 1.0))

    def locate(c, q, valid, shift):
        past = c <= q
        expert = jnp.sum(jnp.where(past, 1.0, 0.0), axis=0, keepdims=True)
        rank = q - jnp.max(jnp.where(past, c, 0.0), axis=0, keepdims=True)
        idx = jnp.where(valid, expert * half + rank + shift, float(n_e * half))
        return idx.astype(jnp.int32), expert, rank

    def main_table(way, shift):
        c = cum[:n_e, way:way + 1]
        k_f = iota((n_e, n_main), 0).astype(F32)
        i_f = iota((1, n_main), 1).astype(F32)
        step = jnp.floor((i_f + 0.5) * (1.0 / b))
        q = served(c, step - 1.0, k_f) + (i_f - step * b)
        valid = q < served(c, step, k_f)
        return locate(c, q, valid, shift) + (valid,)

    def flush_table(way, shift):
        k_f = iota((n_e, 256), 0).astype(F32)
        i_f = iota((1, 256), 1).astype(F32) + base_ref[0].astype(F32)
        both = []
        for c in (cum[:n_e, way:way + 1], cum[n_e:, way:way + 1]):
            done = served(c, float(n_e - 1), k_f)
            both.append((c, done, jnp.max(c, axis=0, keepdims=True) - done))
        second = core.astype(F32)
        out = []
        for (c, done, rest), first in zip(both, (second * both[1][2], (1.0 - second) * both[0][2])):
            i = i_f - first
            valid = (i >= 0) & (i < rest)
            out.append(locate(c, done + i, valid, shift) + (valid,))
        return out

    def one_hot(expert, valid, n):
        return jnp.where((iota((n, expert.shape[1]), 0).astype(F32) == expert) & valid, 1.0, 0.0)

    b_own, _ = flush_table(1, float(half // 2))
    a_own, a_par = flush_table(0, 0.0)
    picks = [(b_own[0], a_own[0], jnp.concatenate([one_hot(a_own[1], a_own[3], n_e), one_hot(a_par[1], a_par[3], n_e),
                                                   jnp.zeros((128 - two, 256), F32)], axis=0),
              jnp.where(a_own[3], a_own[2], a_par[2]))]
    if b:
        m_b, m_a = main_table(1, float(half // 2)), main_table(0, 0.0)
        picks.insert(0, (m_b[0], m_a[0], one_hot(m_a[1], m_a[3], 128), m_a[2]))
    idx_b, idx_a, one, rank = [jnp.concatenate(p, axis=1) for p in zip(*picks)]
    tab_v[...] = jnp.where(iota(tab_v.shape, 0) == 0, idx_b, idx_a)
    to_smem = pltpu.make_async_copy(tab_v, tab_s, tab_sem)
    to_smem.start()

    x_own[2].wait_recv()
    to_c[0].start()
    x_own[3].wait_recv()
    to_c[1].start()

    def columns(a):
        return jnp.transpose(jnp.concatenate([a, jnp.zeros((128 - two, half), F32)], axis=0))

    one = one.astype(BF16)
    same = dot(columns(pos[:, :half]).astype(BF16), one) == rank
    for j, g in enumerate(split3(columns(gate))):
        full = jnp.where(same, dot(g, one), 0.0).astype(BF16)
        for m in range(n_main // 128):
            gm[m, j] = full[:, m * 128:(m + 1) * 128]
        gf[j] = full[:, n_main:]

    to_y.wait_recv()
    to_c[2].start()
    to_x.wait_recv()
    to_c[3].start()
    to_smem.wait()
    x_own[4].wait_recv()
    for c in to_c:
        c.wait_recv()

    def chunk(e):
        slot = lax.rem(e, ring)
        return pltpu.make_async_remote_copy(
            src_ref=send.at[slot], dst_ref=recv.at[pl.ds(pl.multiple_of(e * b, b), b)], send_sem=s_sem.at[slot],
            recv_sem=r_sem.at[e], device_id=peer, device_id_type=MESH)

    n_piece = rows_part // fb + 1

    def span(f):
        return (f * fb, fb) if f < n_piece - 1 else (rows_part, cols_part) if f < n_piece else (flush, extra)

    def swapped(way, f):
        rows = pl.ds(*span(f))
        return pltpu.make_async_remote_copy(
            src_ref=cand.at[way, 1 - core, rows], dst_ref=swap.at[way, rows], send_sem=ds_sem.at[way, f],
            recv_sem=dr_sem.at[way, f], device_id=dev_c, device_id_type=MESH)

    def piece(f):
        rows = pl.ds(f * fb, fb)
        return pltpu.make_async_remote_copy(src_ref=f_send.at[rows], dst_ref=f_recv.at[rows], send_sem=fs_sem.at[f],
                                            recv_sem=fr_sem.at[f], device_id=peer, device_id_type=MESH)

    def col_piece(n):
        at = (pl.ds(rows_part, cols_part), pl.ds(n * wide, wide))
        return pltpu.make_async_remote_copy(src_ref=f_send.at[at], dst_ref=f_recv.at[at], send_sem=cs_sem.at[n],
                                            recv_sem=cr_sem.at[n], device_id=peer, device_id_type=MESH)

    def partial(way, i):
        return o_buf[pl.ds(jnp.clip(tab_s[way, i], 0, n_e * half), 1), :]

    def pack_send(e):
        s = lax.rem(e, ring)
        for r in range(b):
            send[s, r:r + 1, :] = partial(0, e * b + r)

    def pack_own(e):
        first = pl.multiple_of(lax.rem(e * b, 128), b)
        for r in range(b):
            own[pl.ds(first + r, 1), :] = partial(1, e * b + r)

    def combine_main(m):
        @pl.loop(m * (128 // b), (m + 1) * (128 // b))
        def _(e):
            chunk(e).wait_recv()
        for h in range(2):
            cols = slice(h * hw, (h + 1) * hw)
            o = (recv[m * 128:(m + 1) * 128, cols] + own[:, cols]).astype(BF16)
            y_acc[h] += dot(gm[m, 0], o) + dot(gm[m, 1], o) + dot(gm[m, 2], o)

    def combine_flush(rows, cols):
        o = (f_recv[rows, cols] + (cand[0, core, rows, cols] + swap[0, rows, cols])).astype(BF16)
        y_acc[core, :, cols] += dot(gf[0, :, rows], o) + dot(gf[1, :, rows], o) + dot(gf[2, :, rows], o)

    slot_i = iota((half, n_tok), 0).astype(F32)

    @pl.loop(0, n_e)
    def _(e):
        slot = lax.rem(e, depth)
        if b:
            @pl.when(e > ring)
            def _():
                chunk(e - 1 - ring).wait_send()

            @pl.when(e >= 1)
            def _():
                pack_send(e - 1)
                chunk(e - 1).start()
        for c in weights(e, slot):
            c.wait()
        if b:
            pack_own(jnp.maximum(e - lag, 0))
        pick = jnp.where(code[pl.ds(e, 1), :] == slot_i, 1.0, 0.0).astype(BF16)
        xs = dot(pick, x_all[...]).astype(BF16)
        u = dot(xs, w1b[slot])
        v = dot(xs, w3b[slot])
        h = (u * jax.nn.sigmoid(u) * v).astype(BF16)
        o_buf[pl.ds(pl.multiple_of(e * half, half), half), :] = dot(h, w2b[slot])

        @pl.when(e + depth < n_e)
        def _():
            for c in weights(e + depth, slot):
                c.start()

        if b:
            for m in range(n_main // 128 - 1):
                @pl.when(e == (m + 1) * 128 // b - 1 + lag)
                def _():
                    combine_main(m)

    if b:
        chunk(n_e - 1 - ring).wait_send()
        pack_send(n_e - 1)
        chunk(n_e - 1).start()

    def pack_cand(way, f):
        first, n = span(f)

        @pl.loop(0, n // 8)
        def _(g):
            for r in range(8):
                i = first + g * 8 + r
                row = partial(1 - way, n_main + i)
                cand[way, 0, pl.ds(i, 1), :] = row[:, :hw]
                cand[way, 1, pl.ds(i, 1), :] = row[:, hw:]
        swapped(way, f).start()

    def join_send(f):
        swapped(1, f).wait_recv()
        rows = slice(f * fb, (f + 1) * fb) if f < n_piece - 1 else slice(rows_part, flush)
        f_send[rows, :] = cand[1, core, rows, :] + swap[1, rows, :]
        if f < n_piece - 1:
            piece(f).start()
        else:
            for n in range(nb):
                col_piece(n).start()

    def more():
        return [pltpu.make_async_copy(f_send.at[pl.ds(flush, extra)], mb_ref, m_sem.at[0]),
                pltpu.make_async_copy(swap.at[0, pl.ds(flush, extra)], ma_ref, m_sem.at[1]),
                pltpu.make_async_copy(gf, mg_ref, m_sem.at[2])]

    def give(o, n):
        to = lax.rem(ep + o, 4)
        h, cols = (core, pl.ds(n * wide, wide)) if n < nb else (1 - core, pl.ds(0, hw))
        return pltpu.make_async_remote_copy(
            src_ref=y_acc.at[h, pl.ds(pl.multiple_of(to * t_loc, t_loc), t_loc), cols], dst_ref=y_recv.at[3 - o, h, :, cols],
            send_sem=ys_sem.at[o - 1, n], recv_sem=yr_sem.at[3 - o, n], device_id={"tp": tp, "ep": to}, device_id_type=MESH)

    for f in range(2):
        pack_cand(1, f)
    for f in range(n_piece):
        join_send(f)
        if f + 2 < n_piece:
            pack_cand(1, f + 2)
    if b:
        @pl.loop(n_e - lag, n_e)
        def _(e):
            pack_own(e)
        combine_main(n_main // 128 - 1)
    for o in (2, 1, 3):
        give(o, nb).start()
    for f in range(n_piece):
        pack_cand(0, f)
    if extra:
        pack_cand(1, n_piece)
        pack_cand(0, n_piece)
    for f in range(n_piece):
        swapped(0, f).wait_recv()
    if extra:
        rows = slice(flush, flush + extra)
        for way in range(2):
            swapped(way, n_piece).wait_recv()
        f_send[rows, :] = cand[1, core, rows, :] + swap[1, rows, :]
        swap[0, rows, :] = cand[0, core, rows, :] + swap[0, rows, :]
        for c in more():
            c.start()
    for f in range(n_piece - 1):
        piece(f).wait_recv()
    combine_flush(slice(0, rows_part), slice(0, hw))
    for n in range(nb):
        col_piece(n).wait_recv()
        combine_flush(slice(rows_part, flush), slice(n * wide, (n + 1) * wide))
        for o in (2, 1, 3):
            give(o, n).start()
    for n in (nb,) + tuple(range(nb)):
        for o in (1, 3, 2):
            give(o, n).wait_recv()
    mine = pl.ds(pl.multiple_of(near, t_loc), t_loc)
    for h in range(2):
        y = y_acc[h, mine, :]
        for o in (1, 3, 2):
            y = y + y_recv[3 - o, h]
        y_ref[:, h * hw:(h + 1) * hw] = y.astype(y_ref.dtype)

    if b:
        @pl.loop(n_e - ring, n_e)
        def _(e):
            chunk(e).wait_send()
    if extra:
        for way in range(2):
            swapped(way, n_piece).wait_send()
        for c in more():
            c.wait()
    for f in range(n_piece):
        for way in range(2):
            swapped(way, f).wait_send()
        if f < n_piece - 1:
            piece(f).wait_send()
    for n in range(nb + 1):
        if n < nb:
            col_piece(n).wait_send()
        for o in (1, 2, 3):
            give(o, n).wait_send()
    for c in x_own + [to_y, to_x] + to_c:
        c.wait_send()


def moe_call(b, rows_part, cols_part, extra, fb, nb, depth, ring, cid, base, x, route, gates, w1, w3, w2):
    t_loc, d = x.shape
    n_e, _, f = w1.shape
    n_main = n_e * b
    flush = rows_part + cols_part
    half = 4 * t_loc
    n_piece = rows_part // fb
    dma = pltpu.SemaphoreType.DMA
    vm = pl.BlockSpec(memory_space=pltpu.VMEM)
    sm = pl.BlockSpec(memory_space=pltpu.SMEM)
    hbm = pl.BlockSpec(memory_space=pl.ANY)
    return pl.pallas_call(
        functools.partial(moe_kernel, b, rows_part, cols_part, extra, fb, nb, depth, ring),
        out_shape=(jax.ShapeDtypeStruct((t_loc, d), F32), jax.ShapeDtypeStruct((1, 1), jnp.int32),
                   jax.ShapeDtypeStruct((max(extra, 8), d // 2), F32), jax.ShapeDtypeStruct((max(extra, 8), d // 2), F32),
                   jax.ShapeDtypeStruct((3, half, 256), BF16)),
        in_specs=[sm, vm, vm, vm, hbm, hbm, hbm],
        out_specs=(vm, sm, hbm, hbm, hbm),
        scratch_shapes=[
            pltpu.VMEM((2 * half, d), BF16),
            pltpu.VMEM((8,) + route.shape, jnp.int32),
            pltpu.VMEM((8,) + route.shape, F32),
            pltpu.VMEM((2 * half, 2 * half), BF16),
            pltpu.VMEM((n_e, 2 * half), F32),
            pltpu.VMEM((max(n_main // 128, 1), 3, half, 128), BF16),
            pltpu.VMEM((3, half, 256), BF16),
            pltpu.VMEM((8, n_main + 256), jnp.int32),
            pltpu.SMEM((8, n_main + 256), jnp.int32),
            pltpu.VMEM((depth, d, f), BF16),
            pltpu.VMEM((depth, d, f), BF16),
            pltpu.VMEM((depth, f, d), BF16),
            pltpu.VMEM((n_e * half + 8, d), F32),
            pltpu.VMEM((ring, max(b, 8), d), F32),
            pltpu.VMEM((max(n_main, 8), d), F32),
            pltpu.VMEM((128, d), F32),
            pltpu.VMEM((2, half, d // 2), F32),
            pltpu.VMEM((3, 2, t_loc, d // 2), F32),
            pltpu.VMEM((2, 2, flush + extra, d // 2), F32),
            pltpu.VMEM((2, flush + extra, d // 2), F32),
            pltpu.VMEM((flush + extra, d // 2), F32),
            pltpu.VMEM((flush, d // 2), F32),
            dma((2, 8)), dma((2, 8)), dma((11,)), dma((11,)), dma, dma((3, depth)), dma((ring,)), dma((n_e,)),
            dma((2, n_piece + 2)), dma((2, n_piece + 2)), dma((n_piece,)), dma((n_piece,)), dma((nb,)), dma((nb,)),
            dma((3, nb + 1)), dma((3, nb + 1)), dma((3,)),
        ],
        compiler_params=pltpu.CompilerParams(collective_id=cid, has_side_effects=True, vmem_limit_bytes=67043328),
    )(base, x, route, gates, w1, w3, w2)


def more_kernel(first, n_piece, y1_ref, mb_ref, ma_ref, mg_ref, y_ref, recv, acc, y2, y_recv, s_sem, r_sem, ys_sem, yr_sem):
    tp = lax.axis_index("tp")
    ep = lax.axis_index("ep")
    core = lax.rem(ep, 2)
    t_loc, d = y1_ref.shape
    hw = d // 2
    rows, wide = mb_ref.shape[0], hw // n_piece
    peer = {"tp": lax.rem(tp + 1, 2), "ep": ep}
    mates = [{"tp": tp, "ep": lax.rem(ep + o, 4)} for o in (1, 2, 3)]
    barrier = pltpu.get_barrier_semaphore()
    for to in [peer] + mates:
        pl.semaphore_signal(barrier, inc=1, device_id=to, device_id_type=MESH)
    pl.semaphore_wait(barrier, 4)

    def piece(n):
        cols = pl.ds(n * wide, wide)
        return pltpu.make_async_remote_copy(src_ref=mb_ref.at[:, cols], dst_ref=recv.at[:, cols], send_sem=s_sem.at[n],
                                            recv_sem=r_sem.at[n], device_id=peer, device_id_type=MESH)

    def give(o, n):
        to = lax.rem(ep + o, 4)
        cols = pl.ds(n * wide, wide)
        return pltpu.make_async_remote_copy(
            src_ref=acc.at[pl.ds(pl.multiple_of(to * t_loc, t_loc), t_loc), cols], dst_ref=y_recv.at[3 - o, :, cols],
            send_sem=ys_sem.at[o - 1, n], recv_sem=yr_sem.at[3 - o, n], device_id=mates[o - 1], device_id_type=MESH)

    for n in range(n_piece):
        piece(n).start()
    for n in range(n_piece):
        cols = slice(n * wide, (n + 1) * wide)
        piece(n).wait_recv()
        o = (recv[:, cols] + ma_ref[:, cols]).astype(BF16)
        acc[:, cols] = sum(dot(mg_ref[j, :, first:first + rows], o) for j in range(3))
        for o in (2, 1, 3):
            give(o, n).start()
    for h in range(2):
        y2[h] = y1_ref[:, h * hw:(h + 1) * hw]
    for n in range(n_piece):
        for o in (1, 2, 3):
            give(o, n).wait_recv()
    y2[core] += acc[pl.ds(pl.multiple_of(ep * t_loc, t_loc), t_loc), :] + y_recv[1]
    y2[1 - core] += y_recv[0] + y_recv[2]
    for h in range(2):
        y_ref[:, h * hw:(h + 1) * hw] = y2[h]
    for n in range(n_piece):
        piece(n).wait_send()
        for o in (1, 2, 3):
            give(o, n).wait_send()


def more_call(first, n_piece, cid, y1, mb, ma, mg):
    t_loc, d = y1.shape
    dma = pltpu.SemaphoreType.DMA
    vm = pl.BlockSpec(memory_space=pltpu.VMEM)
    return pl.pallas_call(
        functools.partial(more_kernel, first, n_piece),
        out_shape=jax.ShapeDtypeStruct((t_loc, d), F32),
        in_specs=[vm] * 4,
        out_specs=vm,
        scratch_shapes=[
            pltpu.VMEM(mb.shape, F32),
            pltpu.VMEM((4 * t_loc, d // 2), F32),
            pltpu.VMEM((2, t_loc, d // 2), F32),
            pltpu.VMEM((3, t_loc, d // 2), F32),
            dma((n_piece,)), dma((n_piece,)), dma((3, n_piece)), dma((3, n_piece)),
        ],
        compiler_params=pltpu.CompilerParams(collective_id=cid, has_side_effects=True, vmem_limit_bytes=32000000),
    )(y1, mb, ma, mg)


def solution(mesh):
    tok_spec = P(('dp', 'tp', 'ep'), None)

    def local(x, route_idx, gates, w1, w3, w2):
        rt, gt = route_idx.T, gates.T
        zero = jnp.zeros((1,), jnp.int32)
        y1, need, mb, ma, mg = moe_call(8, 80, 64, 96, 16, 8, 3, 4, 1, zero, x, rt, gt, w1, w3, w2)

        def slow(y1, mb, ma, mg):
            part = 192

            def one(p, acc):
                base = jnp.full((1,), p * part, jnp.int32)
                return acc + moe_call(0, part - 64, 64, 0, 32, 8, 3, 4, 2, base, x, rt, gt, w1, w3, w2)[0]

            return lax.fori_loop(0, pl.cdiv(2048, part), one, jnp.zeros(x.shape, F32))

        y = lax.switch(need[0, 0], [lambda y1, mb, ma, mg: y1, functools.partial(more_call, 144, 4, 3), slow], y1, mb, ma, mg)
        return y.astype(BF16)

    return jax.shard_map(local, mesh=mesh,
                         in_specs=(tok_spec, tok_spec, tok_spec, P('ep', None, 'tp'), P('ep', None, 'tp'), P('ep', 'tp', None)),
                         out_specs=tok_spec, check_vma=False)
```

```python
import functools

import jax
import jax.numpy as jnp
from jax import lax
from jax.experimental import pallas as pl
from jax.experimental.pallas import tpu as pltpu
from jax.sharding import PartitionSpec as P

MESH = pl.DeviceIdType.MESH
F32 = jnp.float32
BF16 = jnp.bfloat16
BIG = 1e9


def dot(a, b):
    return jnp.dot(a, b, preferred_element_type=F32)


def iota(shape, dim):
    return lax.broadcasted_iota(jnp.int32, shape, dim)


def split3(g):
    g1 = g.astype(BF16)
    r = g - g1.astype(F32)
    g2 = r.astype(BF16)
    g3 = (r - g2.astype(F32)).astype(BF16)
    return g1, g2, g3


def moe_kernel(b, rows_part, cols_part, extra, fb, nb, depth, ring, *refs):
    (base_ref, x_ref, route_ref, gates_ref, w1_ref, w3_ref, w2_ref, y_ref, need_ref, mb_ref, ma_ref, mg_ref,
     x_all, r_all, g_all, before, code, gm, gf, tab_v, tab_s, w1b, w3b, w2b, o_buf, send, recv, own, y_acc, y_recv,
     cand, swap, f_send, f_recv,
     i_sem, gs_sem, gr_sem, xs_sem, xr_sem, tab_sem, w_sem, s_sem, r_sem, ds_sem, dr_sem, fs_sem, fr_sem, cs_sem, cr_sem,
     ys_sem, yr_sem, m_sem) = refs
    tp = lax.axis_index("tp")
    ep = lax.axis_index("ep")
    t_loc, d = x_ref.shape
    n_e = w1_ref.shape[0]
    half = 4 * t_loc
    n_tok = 2 * half
    flush = rows_part + cols_part
    n_main = n_e * b
    lag = 4
    hw = d // 2
    wide = hw // nb
    core = lax.rem(ep, 2)
    tp_peer = lax.rem(tp + 1, 2)
    ep_x = lax.rem(ep + 2, 4)
    ep_c = ep + 1 - 2 * lax.rem(ep, 2)
    ep_d = lax.rem(ep_c + 2, 4)
    peer = {"tp": tp_peer, "ep": ep}
    dev_x = {"tp": tp, "ep": ep_x}
    dev_c = {"tp": tp, "ep": ep_c}

    def weights(e, slot):
        return [pltpu.make_async_copy(w1_ref.at[e], w1b.at[slot], w_sem.at[0, slot]),
                pltpu.make_async_copy(w3_ref.at[e], w3b.at[slot], w_sem.at[1, slot]),
                pltpu.make_async_copy(w2_ref.at[e], w2b.at[slot], w_sem.at[2, slot])]

    others = [(dt, de) for dt in range(2) for de in range(4) if (dt, de) != (0, 0)]

    def device(dt, de):
        return {"tp": lax.rem(tp + dt, 2), "ep": lax.rem(ep + de, 4)}


    barrier = pltpu.get_barrier_semaphore()
    for dt, de in others:
        pl.semaphore_signal(barrier, inc=1, device_id=device(dt, de), device_id_type=MESH)

    mine = pl.ds(pl.multiple_of(ep * t_loc, t_loc), t_loc)
    inputs = [pltpu.make_async_copy(route_ref, r_all.at[ep], i_sem.at[0]),
              pltpu.make_async_copy(gates_ref, g_all.at[ep], i_sem.at[1]),
              pltpu.make_async_copy(x_ref, x_all.at[mine], i_sem.at[2])]
    for c in inputs:
        c.start()
    t_i, u_i = iota((n_tok, n_tok), 0), iota((n_tok, n_tok), 1)
    before[...] = jnp.where((t_i < u_i) & ((t_i < half) == (u_i < half)), 1.0, 0.0).astype(BF16)
    y_acc[...] = jnp.zeros_like(y_acc)
    o_buf[n_e * half:, :] = jnp.zeros((8, d), F32)
    for c in inputs:
        c.wait()
    for e in range(depth):
        for c in weights(e, e):
            c.start()
    pl.semaphore_wait(barrier, len(others))

    def gather(kind, dt, de):
        dst = (r_all, g_all)[kind]
        return pltpu.make_async_remote_copy(
            src_ref=dst.at[ep], dst_ref=dst.at[dt * 4 + ep], send_sem=gs_sem.at[kind, dt * 4 + de],
            recv_sem=gr_sem.at[kind, dt * 4 + de], device_id=device(dt, de), device_id_type=MESH)

    def rows_of(first, n):
        return x_all.at[pl.ds(pl.multiple_of(first, 16), n)]

    def x_copy(i, src, dst, to):
        return pltpu.make_async_remote_copy(src_ref=src, dst_ref=dst, send_sem=xs_sem.at[i], recv_sem=xr_sem.at[i],
                                            device_id=to, device_id_type=MESH)

    near, far, h_loc = ep * t_loc, half + ep * t_loc, t_loc // 2
    nx = ep_x * t_loc
    x_own = [x_copy(0, rows_of(near, h_loc), rows_of(near, h_loc), dev_x),
             x_copy(1, rows_of(near + h_loc, h_loc), rows_of(far + h_loc, h_loc), peer),
             x_copy(2, rows_of(near + h_loc, h_loc), rows_of(near + h_loc, h_loc), dev_x),
             x_copy(3, rows_of(near, h_loc), rows_of(far, h_loc), peer),
             x_copy(4, rows_of(near, t_loc), rows_of(near, t_loc), dev_c)]

    def passed(i, row, n, to):
        return x_copy(i, rows_of(row, n), rows_of(row, n), to)

    to_y = x_copy(5, rows_of(nx, h_loc), rows_of(half + nx, h_loc), peer)
    to_x = passed(6, far + h_loc, h_loc, dev_x)
    to_c = [passed(7, nx, t_loc, dev_c), passed(8, far, t_loc, dev_c),
            passed(9, half + nx, h_loc, dev_c), passed(10, half + nx + h_loc, h_loc, dev_c)]

    for kind in range(2):
        for dt, de in others:
            gather(kind, dt, de).start()
    for c in x_own:
        c.start()
    for kind in range(2):
        for dt, de in others:
            gather(kind, dt, de).wait()

    x_own[0].wait_recv()
    to_y.start()
    x_own[1].wait_recv()
    to_x.start()

    route = jnp.concatenate([r_all[i] for i in range(8)], axis=1)
    gates = jnp.concatenate([g_all[i] for i in range(4)], axis=1)
    n_all = 4 * n_e
    e_all = iota((n_all, n_tok), 0)
    e_two = iota((2 * n_e, n_tok), 0)
    e_two = jnp.where(e_two < n_e, e_two + ep * n_e, e_two + (ep_c - 1) * n_e)
    hit_all = jnp.zeros((n_all, n_tok), F32)
    hit = jnp.zeros((2 * n_e, n_tok), F32)
    gate = jnp.zeros((2 * n_e, half), F32)
    for k in range(route.shape[0]):
        row = route[k:k + 1, :]
        hit_all = jnp.where(row == e_all, 1.0, hit_all)
        same = row == e_two
        hit = jnp.where(same, 1.0, hit)
        gate = jnp.where(same[:, :half], gates[k:k + 1, :], gate)
    u2, s2 = iota((n_tok, 128), 0), iota((n_tok, 128), 1)
    side = jnp.where((s2 == 0) & (u2 < half) | (s2 == 1) & (u2 >= half), 1.0, 0.0).astype(BF16)
    k_i, s_i = iota((n_all, n_all), 0), iota((n_all, n_all), 1)
    in_block = functools.reduce(lambda a, c: a | c, [(k_i >= i * n_e) & (k_i < (i + 1) * n_e) & (s_i >= i * n_e) & (s_i < (i + 1) * n_e) for i in range(4)])
    suffix = jnp.where((s_i >= k_i) & in_block, 1.0, 0.0).astype(BF16)
    left = dot(suffix, (dot(hit_all.astype(BF16), side) - b).astype(BF16))
    left = [jnp.maximum(jnp.max(left[i * n_e:(i + 1) * n_e], axis=0, keepdims=True), 0.0) for i in range(4)]
    left = jnp.max(jnp.maximum(left[0] + left[1], left[2] + left[3]))
    need_ref[0, 0] = jnp.where(left > flush, 1, 0) + jnp.where(left > flush + extra, 1, 0)

    hit_b = hit.astype(BF16)
    pos = dot(hit_b, before[...])
    code[...] = jnp.where(hit > 0, pos + jnp.where(iota((2 * n_e, n_tok), 1) >= half, float(half // 2), 0.0), -1.0)[:n_e]
    two = 2 * n_e
    up_i, up_j = iota((two, two), 0), iota((two, two), 1)
    upto = jnp.where((up_j <= up_i) & ((up_j < n_e) == (up_i < n_e)), 1.0, 0.0).astype(BF16)
    cum = dot(upto, dot(hit_b, side).astype(BF16))

    def served(c, m, k_f):
        inner = jnp.min(jnp.where(k_f <= m, c + b * (m - k_f), BIG), axis=0, keepdims=True)
        return jnp.minimum(inner, b * (m + 1.0))

    def locate(c, q, valid, shift):
        past = c <= q
        expert = jnp.sum(jnp.where(past, 1.0, 0.0), axis=0, keepdims=True)
        rank = q - jnp.max(jnp.where(past, c, 0.0), axis=0, keepdims=True)
        idx = jnp.where(valid, expert * half + rank + shift, float(n_e * half))
        return idx.astype(jnp.int32), expert, rank

    def main_table(way, shift):
        c = cum[:n_e, way:way + 1]
        k_f = iota((n_e, n_main), 0).astype(F32)
        i_f = iota((1, n_main), 1).astype(F32)
        step = jnp.floor((i_f + 0.5) * (1.0 / b))
        q = served(c, step - 1.0, k_f) + (i_f - step * b)
        valid = q < served(c, step, k_f)
        return locate(c, q, valid, shift) + (valid,)

    def flush_table(way, shift):
        k_f = iota((n_e, 256), 0).astype(F32)
        i_f = iota((1, 256), 1).astype(F32) + base_ref[0].astype(F32)
        both = []
        for c in (cum[:n_e, way:way + 1], cum[n_e:, way:way + 1]):
            done = served(c, float(n_e - 1), k_f)
            both.append((c, done, jnp.max(c, axis=0, keepdims=True) - done))
        second = core.astype(F32)
        out = []
        for (c, done, rest), first in zip(both, (second * both[1][2], (1.0 - second) * both[0][2])):
            i = i_f - first
            valid = (i >= 0) & (i < rest)
            out.append(locate(c, done + i, valid, shift) + (valid,))
        return out

    def one_hot(expert, valid, n):
        return jnp.where((iota((n, expert.shape[1]), 0).astype(F32) == expert) & valid, 1.0, 0.0)

    b_own, _ = flush_table(1, float(half // 2))
    a_own, a_par = flush_table(0, 0.0)
    picks = [(b_own[0], a_own[0], jnp.concatenate([one_hot(a_own[1], a_own[3], n_e), one_hot(a_par[1], a_par[3], n_e),
                                                   jnp.zeros((128 - two, 256), F32)], axis=0),
              jnp.where(a_own[3], a_own[2], a_par[2]))]
    if b:
        m_b, m_a = main_table(1, float(half // 2)), main_table(0, 0.0)
        picks.insert(0, (m_b[0], m_a[0], one_hot(m_a[1], m_a[3], 128), m_a[2]))
    idx_b, idx_a, one, rank = [jnp.concatenate(p, axis=1) for p in zip(*picks)]
    tab_v[...] = jnp.where(iota(tab_v.shape, 0) == 0, idx_b, idx_a)
    to_smem = pltpu.make_async_copy(tab_v, tab_s, tab_sem)
    to_smem.start()

    x_own[2].wait_recv()
    to_c[0].start()
    x_own[3].wait_recv()
    to_c[1].start()

    def columns(a):
        return jnp.transpose(jnp.concatenate([a, jnp.zeros((128 - two, half), F32)], axis=0))

    one = one.astype(BF16)
    same = dot(columns(pos[:, :half]).astype(BF16), one) == rank
    for j, g in enumerate(split3(columns(gate))):
        full = jnp.where(same, dot(g, one), 0.0).astype(BF16)
        for m in range(n_main // 128):
            gm[m, j] = full[:, m * 128:(m + 1) * 128]
        gf[j] = full[:, n_main:]

    to_y.wait_recv()
    to_c[2].start()
    to_x.wait_recv()
    to_c[3].start()
    to_smem.wait()
    x_own[4].wait_recv()
    for c in to_c:
        c.wait_recv()

    def chunk(e):
        slot = lax.rem(e, ring)
        return pltpu.make_async_remote_copy(
            src_ref=send.at[slot], dst_ref=recv.at[pl.ds(pl.multiple_of(e * b, b), b)], send_sem=s_sem.at[slot],
            recv_sem=r_sem.at[e], device_id=peer, device_id_type=MESH)

    n_piece = rows_part // fb + 1

    def span(f):
        return (f * fb, fb) if f < n_piece - 1 else (rows_part, cols_part) if f < n_piece else (flush, extra)

    def swapped(way, f):
        rows = pl.ds(*span(f))
        return pltpu.make_async_remote_copy(
            src_ref=cand.at[way, 1 - core, rows], dst_ref=swap.at[way, rows], send_sem=ds_sem.at[way, f],
            recv_sem=dr_sem.at[way, f], device_id=dev_c, device_id_type=MESH)

    def piece(f):
        rows = pl.ds(f * fb, fb)
        return pltpu.make_async_remote_copy(src_ref=f_send.at[rows], dst_ref=f_recv.at[rows], send_sem=fs_sem.at[f],
                                            recv_sem=fr_sem.at[f], device_id=peer, device_id_type=MESH)

    def col_piece(n):
        at = (pl.ds(rows_part, cols_part), pl.ds(n * wide, wide))
        return pltpu.make_async_remote_copy(src_ref=f_send.at[at], dst_ref=f_recv.at[at], send_sem=cs_sem.at[n],
                                            recv_sem=cr_sem.at[n], device_id=peer, device_id_type=MESH)

    def partial(way, i):
        return o_buf[pl.ds(jnp.clip(tab_s[way, i], 0, n_e * half), 1), :]

    def pack_send(e):
        s = lax.rem(e, ring)
        for r in range(b):
            send[s, r:r + 1, :] = partial(0, e * b + r)

    def pack_own(e):
        first = pl.multiple_of(lax.rem(e * b, 128), b)
        for r in range(b):
            own[pl.ds(first + r, 1), :] = partial(1, e * b + r)

    def combine_main(m):
        @pl.loop(m * (128 // b), (m + 1) * (128 // b))
        def _(e):
            chunk(e).wait_recv()
        for h in range(2):
            cols = slice(h * hw, (h + 1) * hw)
            o = (recv[m * 128:(m + 1) * 128, cols] + own[:, cols]).astype(BF16)
            y_acc[h] += dot(gm[m, 0], o) + dot(gm[m, 1], o) + dot(gm[m, 2], o)

    def combine_flush(rows, cols):
        o = (f_recv[rows, cols] + (cand[0, core, rows, cols] + swap[0, rows, cols])).astype(BF16)
        y_acc[core, :, cols] += dot(gf[0, :, rows], o) + dot(gf[1, :, rows], o) + dot(gf[2, :, rows], o)

    slot_i = iota((half, n_tok), 0).astype(F32)

    @pl.loop(0, n_e)
    def _(e):
        slot = lax.rem(e, depth)
        if b:
            @pl.when(e > ring)
            def _():
                chunk(e - 1 - ring).wait_send()

            @pl.when(e >= 1)
            def _():
                pack_send(e - 1)
                chunk(e - 1).start()
        for c in weights(e, slot):
            c.wait()
        if b:
            pack_own(jnp.maximum(e - lag, 0))
        pick = jnp.where(code[pl.ds(e, 1), :] == slot_i, 1.0, 0.0).astype(BF16)
        xs = dot(pick, x_all[...]).astype(BF16)
        u = dot(xs, w1b[slot])
        v = dot(xs, w3b[slot])
        h = (u * jax.nn.sigmoid(u) * v).astype(BF16)
        o_buf[pl.ds(pl.multiple_of(e * half, half), half), :] = dot(h, w2b[slot])

        @pl.when(e + depth < n_e)
        def _():
            for c in weights(e + depth, slot):
                c.start()

        if b:
            for m in range(n_main // 128 - 1):
                @pl.when(e == (m + 1) * 128 // b - 1 + lag)
                def _():
                    combine_main(m)

    if b:
        chunk(n_e - 1 - ring).wait_send()
        pack_send(n_e - 1)
        chunk(n_e - 1).start()

    def pack_cand(way, f):
        first, n = span(f)

        @pl.loop(0, n // 8)
        def _(g):
            for r in range(8):
                i = first + g * 8 + r
                row = partial(1 - way, n_main + i)
                cand[way, 0, pl.ds(i, 1), :] = row[:, :hw]
                cand[way, 1, pl.ds(i, 1), :] = row[:, hw:]
        swapped(way, f).start()

    def join_send(f):
        swapped(1, f).wait_recv()
        rows = slice(f * fb, (f + 1) * fb) if f < n_piece - 1 else slice(rows_part, flush)
        f_send[rows, :] = cand[1, core, rows, :] + swap[1, rows, :]
        if f < n_piece - 1:
            piece(f).start()
        else:
            for n in range(nb):
                col_piece(n).start()

    def more():
        return [pltpu.make_async_copy(f_send.at[pl.ds(flush, extra)], mb_ref, m_sem.at[0]),
                pltpu.make_async_copy(swap.at[0, pl.ds(flush, extra)], ma_ref, m_sem.at[1]),
                pltpu.make_async_copy(gf, mg_ref, m_sem.at[2])]

    def give(o, n):
        to = lax.rem(ep + o, 4)
        h, cols = (core, pl.ds(n * wide, wide)) if n < nb else (1 - core, pl.ds(0, hw))
        return pltpu.make_async_remote_copy(
            src_ref=y_acc.at[h, pl.ds(pl.multiple_of(to * t_loc, t_loc), t_loc), cols], dst_ref=y_recv.at[3 - o, h, :, cols],
            send_sem=ys_sem.at[o - 1, n], recv_sem=yr_sem.at[3 - o, n], device_id={"tp": tp, "ep": to}, device_id_type=MESH)

    for f in range(2):
        pack_cand(1, f)
    for f in range(n_piece):
        join_send(f)
        if f + 2 < n_piece:
            pack_cand(1, f + 2)
    if b:
        @pl.loop(n_e - lag, n_e)
        def _(e):
            pack_own(e)
        combine_main(n_main // 128 - 1)
    for o in (2, 1, 3):
        give(o, nb).start()
    for f in range(n_piece):
        pack_cand(0, f)
    if extra:
        pack_cand(1, n_piece)
        pack_cand(0, n_piece)
    for f in range(n_piece):
        swapped(0, f).wait_recv()
    if extra:
        rows = slice(flush, flush + extra)
        for way in range(2):
            swapped(way, n_piece).wait_recv()
        f_send[rows, :] = cand[1, core, rows, :] + swap[1, rows, :]
        swap[0, rows, :] = cand[0, core, rows, :] + swap[0, rows, :]
        for c in more():
            c.start()
    for f in range(n_piece - 1):
        piece(f).wait_recv()
    combine_flush(slice(0, rows_part), slice(0, hw))
    for n in range(nb):
        col_piece(n).wait_recv()
        combine_flush(slice(rows_part, flush), slice(n * wide, (n + 1) * wide))
        for o in (2, 1, 3):
            give(o, n).start()
    for n in (nb,) + tuple(range(nb)):
        for o in (1, 3, 2):
            give(o, n).wait_recv()
    for h in range(2):
        y = y_acc[h, mine, :]
        for o in (1, 3, 2):
            y = y + y_recv[3 - o, h]
        y_ref[:, h * hw:(h + 1) * hw] = y.astype(y_ref.dtype)

    if b:
        @pl.loop(n_e - ring, n_e)
        def _(e):
            chunk(e).wait_send()
    if extra:
        for way in range(2):
            swapped(way, n_piece).wait_send()
        for c in more():
            c.wait()
    for f in range(n_piece):
        for way in range(2):
            swapped(way, f).wait_send()
        if f < n_piece - 1:
            piece(f).wait_send()
    for n in range(nb + 1):
        if n < nb:
            col_piece(n).wait_send()
        for o in (1, 2, 3):
            give(o, n).wait_send()
    for c in x_own + [to_y, to_x] + to_c:
        c.wait_send()


def moe_call(b, rows_part, cols_part, extra, fb, nb, depth, ring, cid, base, x, route, gates, w1, w3, w2):
    t_loc, d = x.shape
    n_e, _, f = w1.shape
    n_main = n_e * b
    flush = rows_part + cols_part
    half = 4 * t_loc
    n_piece = rows_part // fb
    dma = pltpu.SemaphoreType.DMA
    vm = pl.BlockSpec(memory_space=pltpu.VMEM)
    sm = pl.BlockSpec(memory_space=pltpu.SMEM)
    hbm = pl.BlockSpec(memory_space=pl.ANY)
    return pl.pallas_call(
        functools.partial(moe_kernel, b, rows_part, cols_part, extra, fb, nb, depth, ring),
        out_shape=(jax.ShapeDtypeStruct((t_loc, d), F32), jax.ShapeDtypeStruct((1, 1), jnp.int32),
                   jax.ShapeDtypeStruct((max(extra, 8), d // 2), F32), jax.ShapeDtypeStruct((max(extra, 8), d // 2), F32),
                   jax.ShapeDtypeStruct((3, half, 256), BF16)),
        in_specs=[sm, hbm, hbm, hbm, hbm, hbm, hbm],
        out_specs=(vm, sm, hbm, hbm, hbm),
        scratch_shapes=[
            pltpu.VMEM((2 * half, d), BF16),
            pltpu.VMEM((8,) + route.shape, jnp.int32),
            pltpu.VMEM((8,) + route.shape, F32),
            pltpu.VMEM((2 * half, 2 * half), BF16),
            pltpu.VMEM((n_e, 2 * half), F32),
            pltpu.VMEM((max(n_main // 128, 1), 3, half, 128), BF16),
            pltpu.VMEM((3, half, 256), BF16),
            pltpu.VMEM((8, n_main + 256), jnp.int32),
            pltpu.SMEM((8, n_main + 256), jnp.int32),
            pltpu.VMEM((depth, d, f), BF16),
            pltpu.VMEM((depth, d, f), BF16),
            pltpu.VMEM((depth, f, d), BF16),
            pltpu.VMEM((n_e * half + 8, d), F32),
            pltpu.VMEM((ring, max(b, 8), d), F32),
            pltpu.VMEM((max(n_main, 8), d), F32),
            pltpu.VMEM((128, d), F32),
            pltpu.VMEM((2, half, d // 2), F32),
            pltpu.VMEM((3, 2, t_loc, d // 2), F32),
            pltpu.VMEM((2, 2, flush + extra, d // 2), F32),
            pltpu.VMEM((2, flush + extra, d // 2), F32),
            pltpu.VMEM((flush + extra, d // 2), F32),
            pltpu.VMEM((flush, d // 2), F32),
            dma((3,)), dma((2, 8)), dma((2, 8)), dma((11,)), dma((11,)), dma, dma((3, depth)), dma((ring,)), dma((n_e,)),
            dma((2, n_piece + 2)), dma((2, n_piece + 2)), dma((n_piece,)), dma((n_piece,)), dma((nb,)), dma((nb,)),
            dma((3, nb + 1)), dma((3, nb + 1)), dma((3,)),
        ],
        compiler_params=pltpu.CompilerParams(collective_id=cid, has_side_effects=True, vmem_limit_bytes=67043328),
    )(base, x, route, gates, w1, w3, w2)


def more_kernel(first, n_piece, y1_ref, mb_ref, ma_ref, mg_ref, y_ref, recv, acc, y2, y_recv, s_sem, r_sem, ys_sem, yr_sem):
    tp = lax.axis_index("tp")
    ep = lax.axis_index("ep")
    core = lax.rem(ep, 2)
    t_loc, d = y1_ref.shape
    hw = d // 2
    rows, wide = mb_ref.shape[0], hw // n_piece
    peer = {"tp": lax.rem(tp + 1, 2), "ep": ep}
    mates = [{"tp": tp, "ep": lax.rem(ep + o, 4)} for o in (1, 2, 3)]
    barrier = pltpu.get_barrier_semaphore()
    for to in [peer] + mates:
        pl.semaphore_signal(barrier, inc=1, device_id=to, device_id_type=MESH)
    pl.semaphore_wait(barrier, 4)

    def piece(n):
        cols = pl.ds(n * wide, wide)
        return pltpu.make_async_remote_copy(src_ref=mb_ref.at[:, cols], dst_ref=recv.at[:, cols], send_sem=s_sem.at[n],
                                            recv_sem=r_sem.at[n], device_id=peer, device_id_type=MESH)

    def give(o, n):
        to = lax.rem(ep + o, 4)
        cols = pl.ds(n * wide, wide)
        return pltpu.make_async_remote_copy(
            src_ref=acc.at[pl.ds(pl.multiple_of(to * t_loc, t_loc), t_loc), cols], dst_ref=y_recv.at[3 - o, :, cols],
            send_sem=ys_sem.at[o - 1, n], recv_sem=yr_sem.at[3 - o, n], device_id=mates[o - 1], device_id_type=MESH)

    for n in range(n_piece):
        piece(n).start()
    for n in range(n_piece):
        cols = slice(n * wide, (n + 1) * wide)
        piece(n).wait_recv()
        o = (recv[:, cols] + ma_ref[:, cols]).astype(BF16)
        acc[:, cols] = sum(dot(mg_ref[j, :, first:first + rows], o) for j in range(3))
        for o in (2, 1, 3):
            give(o, n).start()
    for h in range(2):
        y2[h] = y1_ref[:, h * hw:(h + 1) * hw]
    for n in range(n_piece):
        for o in (1, 2, 3):
            give(o, n).wait_recv()
    y2[core] += acc[pl.ds(pl.multiple_of(ep * t_loc, t_loc), t_loc), :] + y_recv[1]
    y2[1 - core] += y_recv[0] + y_recv[2]
    for h in range(2):
        y_ref[:, h * hw:(h + 1) * hw] = y2[h]
    for n in range(n_piece):
        piece(n).wait_send()
        for o in (1, 2, 3):
            give(o, n).wait_send()


def more_call(first, n_piece, cid, y1, mb, ma, mg):
    t_loc, d = y1.shape
    dma = pltpu.SemaphoreType.DMA
    vm = pl.BlockSpec(memory_space=pltpu.VMEM)
    return pl.pallas_call(
        functools.partial(more_kernel, first, n_piece),
        out_shape=jax.ShapeDtypeStruct((t_loc, d), F32),
        in_specs=[vm] * 4,
        out_specs=vm,
        scratch_shapes=[
            pltpu.VMEM(mb.shape, F32),
            pltpu.VMEM((4 * t_loc, d // 2), F32),
            pltpu.VMEM((2, t_loc, d // 2), F32),
            pltpu.VMEM((3, t_loc, d // 2), F32),
            dma((n_piece,)), dma((n_piece,)), dma((3, n_piece)), dma((3, n_piece)),
        ],
        compiler_params=pltpu.CompilerParams(collective_id=cid, has_side_effects=True, vmem_limit_bytes=32000000),
    )(y1, mb, ma, mg)


def solution(mesh):
    tok_spec = P(('dp', 'tp', 'ep'), None)

    def local(x, route_idx, gates, w1, w3, w2):
        rt, gt = route_idx.T, gates.T
        zero = jnp.zeros((1,), jnp.int32)
        y1, need, mb, ma, mg = moe_call(8, 80, 64, 96, 16, 8, 3, 4, 1, zero, x, rt, gt, w1, w3, w2)

        def slow(y1, mb, ma, mg):
            part = 192

            def one(p, acc):
                base = jnp.full((1,), p * part, jnp.int32)
                return acc + moe_call(0, part - 64, 64, 0, 32, 8, 3, 4, 2, base, x, rt, gt, w1, w3, w2)[0]

            return lax.fori_loop(0, pl.cdiv(2048, part), one, jnp.zeros(x.shape, F32))

        y = lax.switch(need[0, 0], [lambda y1, mb, ma, mg: y1, functools.partial(more_call, 144, 4, 3), slow], y1, mb, ma, mg)
        return y.astype(BF16)

    return jax.shard_map(local, mesh=mesh,
                         in_specs=(tok_spec, tok_spec, tok_spec, P('ep', None, 'tp'), P('ep', None, 'tp'), P('ep', 'tp', None)),
                         out_specs=tok_spec, check_vma=False)
```

```python
import functools

import jax
import jax.numpy as jnp
from jax import lax
from jax.experimental import pallas as pl
from jax.experimental.pallas import tpu as pltpu
from jax.sharding import PartitionSpec as P

MESH = pl.DeviceIdType.MESH
F32 = jnp.float32
BF16 = jnp.bfloat16
BIG = 1e9


def dot(a, b):
    return jnp.dot(a, b, preferred_element_type=F32)


def iota(shape, dim):
    return lax.broadcasted_iota(jnp.int32, shape, dim)


def split3(g):
    g1 = g.astype(BF16)
    r = g - g1.astype(F32)
    g2 = r.astype(BF16)
    g3 = (r - g2.astype(F32)).astype(BF16)
    return g1, g2, g3


def chunk_of(k, skip):
    return k - lax.div(k, skip)


def moe_kernel(skip, b, rows_part, cols_part, some, extra, fb, nb, depth, ring, *refs):
    (base_ref, x_ref, route_ref, gates_ref, w1_ref, w3_ref, w2_ref, y_ref, need_ref, mb_ref, ma_ref, mg_ref,
     x_all, r_all, g_all, before, code, gm, gf, tab_v, tab_s, w1b, w3b, w2b, o_buf, send, recv, own, y_acc, y_recv,
     cand, swap, f_send, f_recv,
     i_sem, gs_sem, gr_sem, xs_sem, xr_sem, tab_sem, w_sem, s_sem, r_sem, ds_sem, dr_sem, fs_sem, fr_sem, cs_sem, cr_sem,
     ys_sem, yr_sem, m_sem) = refs
    tp = lax.axis_index("tp")
    ep = lax.axis_index("ep")
    t_loc, d = x_ref.shape
    n_e = w1_ref.shape[0]
    half = 4 * t_loc
    n_tok = 2 * half
    flush = rows_part + cols_part
    n_chunk = n_e - (n_e - 1) // skip
    n_main = pl.cdiv(n_chunk * b, 128) * 128
    hw = d // 2
    wide = hw // nb
    core = lax.rem(ep, 2)
    tp_peer = lax.rem(tp + 1, 2)
    ep_x = lax.rem(ep + 2, 4)
    ep_c = ep + 1 - 2 * lax.rem(ep, 2)
    ep_d = lax.rem(ep_c + 2, 4)
    peer = {"tp": tp_peer, "ep": ep}
    dev_x = {"tp": tp, "ep": ep_x}
    dev_c = {"tp": tp, "ep": ep_c}

    def weights(e, slot):
        return [pltpu.make_async_copy(w1_ref.at[e], w1b.at[slot], w_sem.at[0, slot]),
                pltpu.make_async_copy(w3_ref.at[e], w3b.at[slot], w_sem.at[1, slot]),
                pltpu.make_async_copy(w2_ref.at[e], w2b.at[slot], w_sem.at[2, slot])]

    others = [(dt, de) for dt in range(2) for de in range(4) if (dt, de) != (0, 0)]

    def device(dt, de):
        return {"tp": lax.rem(tp + dt, 2), "ep": lax.rem(ep + de, 4)}


    barrier = pltpu.get_barrier_semaphore()
    for dt, de in others:
        pl.semaphore_signal(barrier, inc=1, device_id=device(dt, de), device_id_type=MESH)

    mine = pl.ds(pl.multiple_of(ep * t_loc, t_loc), t_loc)
    inputs = [pltpu.make_async_copy(route_ref, r_all.at[ep], i_sem.at[0]),
              pltpu.make_async_copy(gates_ref, g_all.at[ep], i_sem.at[1]),
              pltpu.make_async_copy(x_ref, x_all.at[mine], i_sem.at[2])]
    for c in inputs:
        c.start()
    t_i, u_i = iota((n_tok, n_tok), 0), iota((n_tok, n_tok), 1)
    before[...] = jnp.where((t_i < u_i) & ((t_i < half) == (u_i < half)), 1.0, 0.0).astype(BF16)
    y_acc[...] = jnp.zeros_like(y_acc)
    o_buf[n_e * half:, :] = jnp.zeros((8, d), F32)
    if n_main > n_chunk * b:
        recv[n_chunk * b:, :] = jnp.zeros((n_main - n_chunk * b, d), F32)
    for c in inputs:
        c.wait()
    for e in range(depth):
        for c in weights(e, e):
            c.start()
    pl.semaphore_wait(barrier, len(others))

    def gather(kind, dt, de):
        dst = (r_all, g_all)[kind]
        return pltpu.make_async_remote_copy(
            src_ref=dst.at[ep], dst_ref=dst.at[dt * 4 + ep], send_sem=gs_sem.at[kind, dt * 4 + de],
            recv_sem=gr_sem.at[kind, dt * 4 + de], device_id=device(dt, de), device_id_type=MESH)

    def rows_of(first, n):
        return x_all.at[pl.ds(pl.multiple_of(first, 16), n)]

    def x_copy(i, src, dst, to):
        return pltpu.make_async_remote_copy(src_ref=src, dst_ref=dst, send_sem=xs_sem.at[i], recv_sem=xr_sem.at[i],
                                            device_id=to, device_id_type=MESH)

    near, far, h_loc = ep * t_loc, half + ep * t_loc, t_loc // 2
    nx = ep_x * t_loc
    x_own = [x_copy(0, rows_of(near, h_loc), rows_of(near, h_loc), dev_x),
             x_copy(1, rows_of(near + h_loc, h_loc), rows_of(far + h_loc, h_loc), peer),
             x_copy(2, rows_of(near + h_loc, h_loc), rows_of(near + h_loc, h_loc), dev_x),
             x_copy(3, rows_of(near, h_loc), rows_of(far, h_loc), peer),
             x_copy(4, rows_of(near, t_loc), rows_of(near, t_loc), dev_c)]

    def passed(i, row, n, to):
        return x_copy(i, rows_of(row, n), rows_of(row, n), to)

    to_y = x_copy(5, rows_of(nx, h_loc), rows_of(half + nx, h_loc), peer)
    to_x = passed(6, far + h_loc, h_loc, dev_x)
    to_c = [passed(7, nx, t_loc, dev_c), passed(8, far, t_loc, dev_c),
            passed(9, half + nx, h_loc, dev_c), passed(10, half + nx + h_loc, h_loc, dev_c)]

    for kind in range(2):
        for dt, de in others:
            gather(kind, dt, de).start()
    for c in x_own:
        c.start()
    for kind in range(2):
        for dt, de in others:
            gather(kind, dt, de).wait()

    x_own[0].wait_recv()
    to_y.start()
    x_own[1].wait_recv()
    to_x.start()

    route = jnp.concatenate([r_all[i] for i in range(8)], axis=1)
    gates = jnp.concatenate([g_all[i] for i in range(4)], axis=1)
    n_all = 4 * n_e
    e_all = iota((n_all, n_tok), 0)
    e_two = iota((2 * n_e, n_tok), 0)
    e_two = jnp.where(e_two < n_e, e_two + ep * n_e, e_two + (ep_c - 1) * n_e)
    hit_all = jnp.zeros((n_all, n_tok), F32)
    hit = jnp.zeros((2 * n_e, n_tok), F32)
    gate = jnp.zeros((2 * n_e, half), F32)
    for k in range(route.shape[0]):
        row = route[k:k + 1, :]
        hit_all = jnp.where(row == e_all, 1.0, hit_all)
        same = row == e_two
        hit = jnp.where(same, 1.0, hit)
        gate = jnp.where(same[:, :half], gates[k:k + 1, :], gate)
    u2, s2 = iota((n_tok, 128), 0), iota((n_tok, 128), 1)
    side = jnp.where((s2 == 0) & (u2 < half) | (s2 == 1) & (u2 >= half), 1.0, 0.0).astype(BF16)
    k_i, s_i = iota((n_all, n_all), 0), iota((n_all, n_all), 1)
    in_block = functools.reduce(lambda a, c: a | c, [(k_i >= i * n_e) & (k_i < (i + 1) * n_e) & (s_i >= i * n_e) & (s_i < (i + 1) * n_e) for i in range(4)])
    suffix = jnp.where((s_i >= k_i) & in_block, 1.0, 0.0).astype(BF16)
    at = iota((n_all, 128), 0).astype(F32)
    at = at - n_e * jnp.floor((at + 0.5) * (1.0 / n_e))
    sends = jnp.where((at > 0) & (at == skip * jnp.floor((at + 0.5) * (1.0 / skip))), 0.0, float(b))
    left = dot(suffix, (dot(hit_all.astype(BF16), side) - sends).astype(BF16))
    left = [jnp.maximum(jnp.max(left[i * n_e:(i + 1) * n_e], axis=0, keepdims=True), 0.0) for i in range(4)]
    left = jnp.max(jnp.maximum(left[0] + left[1], left[2] + left[3]))
    need_ref[0, 0] = sum(jnp.where(left > flush + m, 1, 0) for m in (0, some, extra))

    hit_b = hit.astype(BF16)
    pos = dot(hit_b, before[...])
    code[...] = jnp.where(hit > 0, pos + jnp.where(iota((2 * n_e, n_tok), 1) >= half, float(half // 2), 0.0), -1.0)[:n_e]
    two = 2 * n_e
    up_i, up_j = iota((two, two), 0), iota((two, two), 1)
    upto = jnp.where((up_j <= up_i) & ((up_j < n_e) == (up_i < n_e)), 1.0, 0.0).astype(BF16)
    cum = dot(upto, dot(hit_b, side).astype(BF16))

    def served(c, m, k_f):
        k_f = k_f - jnp.floor((k_f + 0.5) * (1.0 / skip))
        inner = jnp.min(jnp.where(k_f <= m, c + b * (m - k_f), BIG), axis=0, keepdims=True)
        return jnp.minimum(inner, b * (m + 1.0))

    def locate(c, q, valid, shift):
        past = c <= q
        expert = jnp.sum(jnp.where(past, 1.0, 0.0), axis=0, keepdims=True)
        rank = q - jnp.max(jnp.where(past, c, 0.0), axis=0, keepdims=True)
        idx = jnp.where(valid, expert * half + rank + shift, float(n_e * half))
        return idx.astype(jnp.int32), expert, rank

    def main_table(way, shift):
        c = cum[:n_e, way:way + 1]
        k_f = iota((n_e, n_main), 0).astype(F32)
        i_f = iota((1, n_main), 1).astype(F32)
        step = jnp.floor((i_f + 0.5) * (1.0 / b))
        q = served(c, step - 1.0, k_f) + (i_f - step * b)
        valid = (q < served(c, step, k_f)) & (step < n_chunk)
        return locate(c, q, valid, shift) + (valid,)

    def flush_table(way, shift):
        k_f = iota((n_e, 256), 0).astype(F32)
        i_f = iota((1, 256), 1).astype(F32) + base_ref[0].astype(F32)
        both = []
        for c in (cum[:n_e, way:way + 1], cum[n_e:, way:way + 1]):
            done = served(c, float(n_chunk - 1), k_f)
            both.append((c, done, jnp.max(c, axis=0, keepdims=True) - done))
        second = core.astype(F32)
        out = []
        for (c, done, rest), first in zip(both, (second * both[1][2], (1.0 - second) * both[0][2])):
            i = i_f - first
            valid = (i >= 0) & (i < rest)
            out.append(locate(c, done + i, valid, shift) + (valid,))
        return out

    def one_hot(expert, valid, n):
        return jnp.where((iota((n, expert.shape[1]), 0).astype(F32) == expert) & valid, 1.0, 0.0)

    b_own, _ = flush_table(1, float(half // 2))
    a_own, a_par = flush_table(0, 0.0)
    picks = [(b_own[0], a_own[0], jnp.concatenate([one_hot(a_own[1], a_own[3], n_e), one_hot(a_par[1], a_par[3], n_e),
                                                   jnp.zeros((128 - two, 256), F32)], axis=0),
              jnp.where(a_own[3], a_own[2], a_par[2]))]
    if b:
        m_b, m_a = main_table(1, float(half // 2)), main_table(0, 0.0)
        picks.insert(0, (m_b[0], m_a[0], one_hot(m_a[1], m_a[3], 128), m_a[2]))
    idx_b, idx_a, one, rank = [jnp.concatenate(p, axis=1) for p in zip(*picks)]
    tab_v[...] = jnp.where(iota(tab_v.shape, 0) == 0, idx_b, idx_a)
    to_smem = pltpu.make_async_copy(tab_v, tab_s, tab_sem)
    to_smem.start()

    x_own[2].wait_recv()
    to_c[0].start()
    x_own[3].wait_recv()
    to_c[1].start()

    def columns(a):
        return jnp.transpose(jnp.concatenate([a, jnp.zeros((128 - two, half), F32)], axis=0))

    one = one.astype(BF16)
    same = dot(columns(pos[:, :half]).astype(BF16), one) == rank
    for j, g in enumerate(split3(columns(gate))):
        full = jnp.where(same, dot(g, one), 0.0).astype(BF16)
        for m in range(n_main // 128):
            gm[m, j] = full[:, m * 128:(m + 1) * 128]
        gf[j] = full[:, n_main:]

    to_y.wait_recv()
    to_c[2].start()
    to_x.wait_recv()
    to_c[3].start()
    to_smem.wait()
    x_own[4].wait_recv()
    for c in to_c:
        c.wait_recv()

    def chunk(e):
        slot = lax.rem(e, ring)
        return pltpu.make_async_remote_copy(
            src_ref=send.at[slot], dst_ref=recv.at[pl.ds(pl.multiple_of(e * b, b), b)], send_sem=s_sem.at[slot],
            recv_sem=r_sem.at[e], device_id=peer, device_id_type=MESH)

    n_piece = rows_part // fb + 1

    def span(f):
        return (f * fb, fb) if f < n_piece - 1 else (rows_part, cols_part) if f < n_piece else (flush, extra)

    def swapped(way, f):
        rows = pl.ds(*span(f))
        return pltpu.make_async_remote_copy(
            src_ref=cand.at[way, 1 - core, rows], dst_ref=swap.at[way, rows], send_sem=ds_sem.at[way, f],
            recv_sem=dr_sem.at[way, f], device_id=dev_c, device_id_type=MESH)

    def piece(f):
        rows = pl.ds(f * fb, fb)
        return pltpu.make_async_remote_copy(src_ref=f_send.at[rows], dst_ref=f_recv.at[rows], send_sem=fs_sem.at[f],
                                            recv_sem=fr_sem.at[f], device_id=peer, device_id_type=MESH)

    def col_piece(n):
        at = (pl.ds(rows_part, cols_part), pl.ds(n * wide, wide))
        return pltpu.make_async_remote_copy(src_ref=f_send.at[at], dst_ref=f_recv.at[at], send_sem=cs_sem.at[n],
                                            recv_sem=cr_sem.at[n], device_id=peer, device_id_type=MESH)

    def partial(way, i):
        return o_buf[pl.ds(jnp.clip(tab_s[way, i], 0, n_e * half), 1), :]

    def pack_send(e):
        s = lax.rem(e, ring)
        for r in range(b):
            send[s, r:r + 1, :] = partial(0, e * b + r)

    def pack_own(e):
        first = pl.multiple_of(lax.rem(e * b, 128), b)
        for r in range(b):
            own[pl.ds(first + r, 1), :] = partial(1, e * b + r)

    def combine_main(m):
        @pl.loop(m * (128 // b), min((m + 1) * (128 // b), n_chunk))
        def _(e):
            chunk(e).wait_recv()
        for h in range(2):
            cols = slice(h * hw, (h + 1) * hw)
            o = (recv[m * 128:(m + 1) * 128, cols] + own[:, cols]).astype(BF16)
            y_acc[h] += dot(gm[m, 0], o) + dot(gm[m, 1], o) + dot(gm[m, 2], o)

    def combine_flush(rows, cols):
        o = (f_recv[rows, cols] + (cand[0, core, rows, cols] + swap[0, rows, cols])).astype(BF16)
        y_acc[core, :, cols] += dot(gf[0, :, rows], o) + dot(gf[1, :, rows], o) + dot(gf[2, :, rows], o)

    slot_i = iota((half, n_tok), 0).astype(F32)

    @pl.loop(0, n_e)
    def _(e):
        slot = lax.rem(e, depth)
        if b:
            @pl.when((e == 1) | ((e > 1) & (lax.rem(e - 1, skip) != 0)))
            def _():
                c = chunk_of(e - 1, skip)

                @pl.when(c >= ring)
                def _():
                    chunk(c - ring).wait_send()
                pack_send(c)
                chunk(c).start()
        for c in weights(e, slot):
            c.wait()
        pick = jnp.where(code[pl.ds(e, 1), :] == slot_i, 1.0, 0.0).astype(BF16)
        xs = dot(pick, x_all[...]).astype(BF16)
        u = dot(xs, w1b[slot])
        v = dot(xs, w3b[slot])
        h = (u * jax.nn.sigmoid(u) * v).astype(BF16)
        o_buf[pl.ds(pl.multiple_of(e * half, half), half), :] = dot(h, w2b[slot])

        @pl.when(e + depth < n_e)
        def _():
            for c in weights(e + depth, slot):
                c.start()

    if b:
        chunk(n_chunk - 1 - ring).wait_send()
        pack_send(n_chunk - 1)
        chunk(n_chunk - 1).start()

    def pack_cand(way, f):
        first, n = span(f)

        @pl.loop(0, n // 8)
        def _(g):
            for r in range(8):
                i = first + g * 8 + r
                row = partial(1 - way, n_main + i)
                cand[way, 0, pl.ds(i, 1), :] = row[:, :hw]
                cand[way, 1, pl.ds(i, 1), :] = row[:, hw:]
        swapped(way, f).start()

    def join_send(f):
        swapped(1, f).wait_recv()
        rows = slice(f * fb, (f + 1) * fb) if f < n_piece - 1 else slice(rows_part, flush)
        f_send[rows, :] = cand[1, core, rows, :] + swap[1, rows, :]
        if f < n_piece - 1:
            piece(f).start()
        else:
            for n in range(nb):
                col_piece(n).start()

    def more():
        return [pltpu.make_async_copy(f_send.at[pl.ds(flush, extra)], mb_ref, m_sem.at[0]),
                pltpu.make_async_copy(swap.at[0, pl.ds(flush, extra)], ma_ref, m_sem.at[1]),
                pltpu.make_async_copy(gf, mg_ref, m_sem.at[2])]

    def give(o, n):
        to = lax.rem(ep + o, 4)
        h, cols = (core, pl.ds(n * wide, wide)) if n < nb else (1 - core, pl.ds(0, hw))
        return pltpu.make_async_remote_copy(
            src_ref=y_acc.at[h, pl.ds(pl.multiple_of(to * t_loc, t_loc), t_loc), cols], dst_ref=y_recv.at[3 - o, h, :, cols],
            send_sem=ys_sem.at[o - 1, n], recv_sem=yr_sem.at[3 - o, n], device_id={"tp": tp, "ep": to}, device_id_type=MESH)

    for f in range(2):
        pack_cand(1, f)
    for f in range(n_piece):
        join_send(f)
        if f + 2 < n_piece:
            pack_cand(1, f + 2)
    for m in range(n_main // 128):
        @pl.loop(m * (128 // b), min((m + 1) * (128 // b), n_chunk))
        def _(c):
            pack_own(c)
        combine_main(m)
    for o in (2, 1, 3):
        give(o, nb).start()
    for f in range(n_piece):
        pack_cand(0, f)
    if extra:
        pack_cand(1, n_piece)
        pack_cand(0, n_piece)
    for f in range(n_piece):
        swapped(0, f).wait_recv()
    if extra:
        rows = slice(flush, flush + extra)
        for way in range(2):
            swapped(way, n_piece).wait_recv()
        f_send[rows, :] = cand[1, core, rows, :] + swap[1, rows, :]
        swap[0, rows, :] = cand[0, core, rows, :] + swap[0, rows, :]
        for c in more():
            c.start()
    for f in range(n_piece - 1):
        piece(f).wait_recv()
    combine_flush(slice(0, rows_part), slice(0, hw))
    for n in range(nb):
        col_piece(n).wait_recv()
        combine_flush(slice(rows_part, flush), slice(n * wide, (n + 1) * wide))
        for o in (2, 1, 3):
            give(o, n).start()
    for n in (nb,) + tuple(range(nb)):
        for o in (1, 3, 2):
            give(o, n).wait_recv()
    for h in range(2):
        y = y_acc[h, mine, :]
        for o in (1, 3, 2):
            y = y + y_recv[3 - o, h]
        y_ref[:, h * hw:(h + 1) * hw] = y.astype(y_ref.dtype)

    if b:
        @pl.loop(n_chunk - ring, n_chunk)
        def _(e):
            chunk(e).wait_send()
    if extra:
        for way in range(2):
            swapped(way, n_piece).wait_send()
        for c in more():
            c.wait()
    for f in range(n_piece):
        for way in range(2):
            swapped(way, f).wait_send()
        if f < n_piece - 1:
            piece(f).wait_send()
    for n in range(nb + 1):
        if n < nb:
            col_piece(n).wait_send()
        for o in (1, 2, 3):
            give(o, n).wait_send()
    for c in x_own + [to_y, to_x] + to_c:
        c.wait_send()


def moe_call(skip, b, rows_part, cols_part, some, extra, fb, nb, depth, ring, cid, base, x, route, gates, w1, w3, w2):
    t_loc, d = x.shape
    n_e, _, f = w1.shape
    n_main = pl.cdiv((n_e - (n_e - 1) // skip) * b, 128) * 128
    flush = rows_part + cols_part
    half = 4 * t_loc
    n_piece = rows_part // fb
    dma = pltpu.SemaphoreType.DMA
    vm = pl.BlockSpec(memory_space=pltpu.VMEM)
    sm = pl.BlockSpec(memory_space=pltpu.SMEM)
    hbm = pl.BlockSpec(memory_space=pl.ANY)
    return pl.pallas_call(
        functools.partial(moe_kernel, skip, b, rows_part, cols_part, some, extra, fb, nb, depth, ring),
        out_shape=(jax.ShapeDtypeStruct((t_loc, d), F32), jax.ShapeDtypeStruct((1, 1), jnp.int32),
                   jax.ShapeDtypeStruct((max(extra, 8), d // 2), F32), jax.ShapeDtypeStruct((max(extra, 8), d // 2), F32),
                   jax.ShapeDtypeStruct((3, half, 256), BF16)),
        in_specs=[sm, hbm, hbm, hbm, hbm, hbm, hbm],
        out_specs=(vm, sm, hbm, hbm, hbm),
        scratch_shapes=[
            pltpu.VMEM((2 * half, d), BF16),
            pltpu.VMEM((8,) + route.shape, jnp.int32),
            pltpu.VMEM((8,) + route.shape, F32),
            pltpu.VMEM((2 * half, 2 * half), BF16),
            pltpu.VMEM((n_e, 2 * half), F32),
            pltpu.VMEM((max(n_main // 128, 1), 3, half, 128), BF16),
            pltpu.VMEM((3, half, 256), BF16),
            pltpu.VMEM((8, n_main + 256), jnp.int32),
            pltpu.SMEM((8, n_main + 256), jnp.int32),
            pltpu.VMEM((depth, d, f), BF16),
            pltpu.VMEM((depth, d, f), BF16),
            pltpu.VMEM((depth, f, d), BF16),
            pltpu.VMEM((n_e * half + 8, d), F32),
            pltpu.VMEM((ring, max(b, 8), d), F32),
            pltpu.VMEM((max(n_main, 8), d), F32),
            pltpu.VMEM((128, d), F32),
            pltpu.VMEM((2, half, d // 2), F32),
            pltpu.VMEM((3, 2, t_loc, d // 2), F32),
            pltpu.VMEM((2, 2, flush + extra, d // 2), F32),
            pltpu.VMEM((2, flush + extra, d // 2), F32),
            pltpu.VMEM((flush + extra, d // 2), F32),
            pltpu.VMEM((flush, d // 2), F32),
            dma((3,)), dma((2, 8)), dma((2, 8)), dma((11,)), dma((11,)), dma, dma((3, depth)), dma((ring,)), dma((n_e,)),
            dma((2, n_piece + 2)), dma((2, n_piece + 2)), dma((n_piece,)), dma((n_piece,)), dma((nb,)), dma((nb,)),
            dma((3, nb + 1)), dma((3, nb + 1)), dma((3,)),
        ],
        compiler_params=pltpu.CompilerParams(collective_id=cid, has_side_effects=True, vmem_limit_bytes=67043328),
    )(base, x, route, gates, w1, w3, w2)


def more_kernel(first, rows, n_piece, y1_ref, mb_ref, ma_ref, mg_ref, y_ref, recv, acc, y2, y_recv, s_sem, r_sem, ys_sem, yr_sem):
    tp = lax.axis_index("tp")
    ep = lax.axis_index("ep")
    core = lax.rem(ep, 2)
    t_loc, d = y1_ref.shape
    hw = d // 2
    wide = hw // n_piece
    peer = {"tp": lax.rem(tp + 1, 2), "ep": ep}
    mates = [{"tp": tp, "ep": lax.rem(ep + o, 4)} for o in (1, 2, 3)]
    barrier = pltpu.get_barrier_semaphore()
    for to in [peer] + mates:
        pl.semaphore_signal(barrier, inc=1, device_id=to, device_id_type=MESH)
    pl.semaphore_wait(barrier, 4)

    def piece(n):
        cols = pl.ds(n * wide, wide)
        return pltpu.make_async_remote_copy(src_ref=mb_ref.at[pl.ds(0, rows), cols], dst_ref=recv.at[:, cols], send_sem=s_sem.at[n],
                                            recv_sem=r_sem.at[n], device_id=peer, device_id_type=MESH)

    def give(o, n):
        to = lax.rem(ep + o, 4)
        cols = pl.ds(n * wide, wide)
        return pltpu.make_async_remote_copy(
            src_ref=acc.at[pl.ds(pl.multiple_of(to * t_loc, t_loc), t_loc), cols], dst_ref=y_recv.at[3 - o, :, cols],
            send_sem=ys_sem.at[o - 1, n], recv_sem=yr_sem.at[3 - o, n], device_id=mates[o - 1], device_id_type=MESH)

    for n in range(n_piece):
        piece(n).start()
    for n in range(n_piece):
        cols = slice(n * wide, (n + 1) * wide)
        piece(n).wait_recv()
        o = (recv[:, cols] + ma_ref[:rows, cols]).astype(BF16)
        acc[:, cols] = sum(dot(mg_ref[j, :, first:first + rows], o) for j in range(3))
        for o in (2, 1, 3):
            give(o, n).start()
    for h in range(2):
        y2[h] = y1_ref[:, h * hw:(h + 1) * hw]
    for n in range(n_piece):
        for o in (1, 2, 3):
            give(o, n).wait_recv()
    y2[core] += acc[pl.ds(pl.multiple_of(ep * t_loc, t_loc), t_loc), :] + y_recv[1]
    y2[1 - core] += y_recv[0] + y_recv[2]
    for h in range(2):
        y_ref[:, h * hw:(h + 1) * hw] = y2[h]
    for n in range(n_piece):
        piece(n).wait_send()
        for o in (1, 2, 3):
            give(o, n).wait_send()


def more_call(first, rows, n_piece, cid, y1, mb, ma, mg):
    t_loc, d = y1.shape
    dma = pltpu.SemaphoreType.DMA
    vm = pl.BlockSpec(memory_space=pltpu.VMEM)
    return pl.pallas_call(
        functools.partial(more_kernel, first, rows, n_piece),
        out_shape=jax.ShapeDtypeStruct((t_loc, d), F32),
        in_specs=[vm] * 4,
        out_specs=vm,
        scratch_shapes=[
            pltpu.VMEM((rows, d // 2), F32),
            pltpu.VMEM((4 * t_loc, d // 2), F32),
            pltpu.VMEM((2, t_loc, d // 2), F32),
            pltpu.VMEM((3, t_loc, d // 2), F32),
            dma((n_piece,)), dma((n_piece,)), dma((3, n_piece)), dma((3, n_piece)),
        ],
        compiler_params=pltpu.CompilerParams(collective_id=cid, has_side_effects=True, vmem_limit_bytes=32000000),
    )(y1, mb, ma, mg)


def solution(mesh):
    tok_spec = P(('dp', 'tp', 'ep'), None)

    def local(x, route_idx, gates, w1, w3, w2):
        rt, gt = route_idx.T, gates.T
        zero = jnp.zeros((1,), jnp.int32)
        y1, need, mb, ma, mg = moe_call(11, 8, 96, 64, 48, 80, 16, 8, 3, 4, 1, zero, x, rt, gt, w1, w3, w2)

        def slow(y1, mb, ma, mg):
            part = 192

            def one(p, acc):
                base = jnp.full((1,), p * part, jnp.int32)
                return acc + moe_call(8, 0, part - 64, 64, 0, 0, 32, 8, 3, 4, 2, base, x, rt, gt, w1, w3, w2)[0]

            return lax.fori_loop(0, pl.cdiv(2048, part), one, jnp.zeros(x.shape, F32))

        y = lax.switch(need[0, 0], [lambda y1, mb, ma, mg: y1, functools.partial(more_call, 160, 48, 4, 3), functools.partial(more_call, 160, 80, 4, 4), slow], y1, mb, ma, mg)
        return y.astype(BF16)

    return jax.shard_map(local, mesh=mesh,
                         in_specs=(tok_spec, tok_spec, tok_spec, P('ep', None, 'tp'), P('ep', None, 'tp'), P('ep', 'tp', None)),
                         out_specs=tok_spec, check_vma=False)
```
